256 devices in a mesh: tm: 128 (over z, y, x_lo, core), gen: 2 (over x_hi).
Axes of the slice: x: 4 (x_hi: 2, x_lo: 2; x = x_hi * 2 + x_lo), y: 4, z: 8, core: 2. Of those that a mesh axis runs over, the one named last changes fastest.
Arguments:
- dispatch: float32 [12288, 8192], P('tm', 'gen'), may hold values from 0 to 2
- cost: float32 [8192], P('gen'), may hold values from -4 to 4
- p_low: float32 [8192], P('gen'), may hold values from 0 to 0.4
- p_high: float32 [8192], P('gen'), may hold values from 1.2 to 2.5
- ramp_limit: float32 [8192], P('gen'), may hold values from 0.05 to 1
- p_init: float32 [8192], P('gen'), may hold values from 0 to 2
- demand: float32 [12288], P('tm'), may hold values from 70 to 110
- bus_of: int32 [8192], P('gen'), may hold values from 0 to 2047
- ptdf: bfloat16 [1024, 2048], replicated, may hold values from -0.0625 to 0.0625
- line_base: float32 [12288, 1024], P('tm', 'gen'), may hold values from -6 to 6
- line_limit: float32 [1024], P('gen'), may hold values from 0.2 to 2
- line_dual: float32 [12288, 1024], P('tm', 'gen'), may hold values from -3 to 3
- ramp_dual: float32 [12288, 8192], P('tm', 'gen'), may hold values from -3 to 3
- balance_dual: float32 [12288], P('tm'), may hold values from -5 to 5
Outputs:
- dispatch_out: float32 [12288, 8192], P('tm', 'gen')
- line_dual_out: float32 [12288, 1024], P('tm', 'gen')
- ramp_dual_out: float32 [12288, 8192], P('tm', 'gen')
- balance_dual_out: float32 [12288], P('tm')
- movement: float32 [2, 2], replicated
The draws below stay inside these ranges and needn't reach their ends.
Inputs may be any that keep to these rules, and one draw needn't show every extreme that they name: `bus_of`: each generator's bus.
All inputs are finite; a program needn't handle non-finite values.
Results may differ from the reference program's by a relative error of at most 0.0011.
Values may be sent and summed in bfloat16 or wider, within the bound.
A program may use at most 64 MiB of HBM per device.

```python
import math
import jax
import jax.numpy as jnp
from jax import lax

G = 8192
L = 1024
B = 2048
ITERS = 2
HOURS = 12288


def set_ends(result, own_key, low, top_value):
    longest = result.shape.index(max(result.shape))
    spots = []
    for shift in (0, 1):
        where = [jax.random.randint(jax.random.fold_in(own_key, axis), (), 0, length) for axis, length in enumerate(result.shape)]
        where[longest] = (where[longest] + shift) % result.shape[longest]
        spots.append(tuple(where))
    return result.at[spots[0]].set(low).at[spots[1]].set(top_value)


def level_of(own_key, dims, pieces, smallest, high):
    def one(dim, blocks):
        heights = jax.random.uniform(jax.random.fold_in(jax.random.fold_in(own_key, 6), dim), (blocks,), jnp.float32, smallest / len(pieces), high / len(pieces))
        return jnp.repeat(jnp.exp(heights), dims[dim] // blocks).reshape((-1,) + (1,) * (len(dims) - dim - 1))

    factor_of = one(*pieces[0])
    for cut in pieces[1:]:
        factor_of = factor_of * one(*cut)
    return factor_of


def centred(key, shape, spread, limit, shards=(), kind=jnp.bfloat16):
    drawn = spread * jax.random.normal(key, shape, jnp.float32)
    if shards:
        drawn = drawn * level_of(key, shape, shards, -0.22, 0.18)
    return jnp.clip(drawn, -limit, limit).astype(kind)


def setup_inputs(seed: int = 0) -> dict:
    keys = jax.random.split(jax.random.key(seed), 15)
    return {
        "dispatch": jnp.clip(2.0 * jax.random.uniform(keys[0], (HOURS, G), jnp.float32) ** level_of(keys[0], (HOURS, G), ((0, 128), (1, 2)), -0.2, 0.2), 0.0, 2.0),
        "cost": centred(keys[1], (G,), 1.0, 4.0, ((0, 2),), jnp.float32),
        "p_low": jnp.clip(0.4 * jax.random.uniform(keys[2], (G,), jnp.float32) ** level_of(keys[2], (G,), ((0, 2),), -0.2, 0.2), 0.0, 0.4),
        "p_high": jnp.clip(1.2 + 1.3 * jax.random.uniform(keys[3], (G,), jnp.float32) ** level_of(keys[3], (G,), ((0, 2),), -0.2, 0.2), 1.2, 2.5),
        "ramp_limit": jnp.clip(jnp.exp(math.log(1.0) - 2.9957323 * jax.random.uniform(keys[4], (G,), jnp.float32) ** level_of(keys[4], (G,), ((0, 2),), -0.2, 0.2)), 0.05, 1.0),
        "p_init": jnp.clip(2.0 * jax.random.uniform(keys[5], (G,), jnp.float32) ** level_of(keys[5], (G,), ((0, 2),), -0.2, 0.2), 0.0, 2.0),
        "demand": jnp.clip(70.0 + 40.0 * jax.random.uniform(keys[6], (HOURS,), jnp.float32) ** level_of(keys[6], (HOURS,), ((0, 128),), -0.2, 0.2), 70.0, 110.0),
        "bus_of": set_ends(jax.random.randint(keys[7], (G,), 0, B), jax.random.fold_in(keys[7], 1), 0, B - 1).astype(jnp.int32),
        "ptdf": centred(keys[8], (L, B), G ** -0.5, 0.0625),
        "line_base": centred(keys[9], (HOURS, L), 1.0, 6.0, ((0, 128), (1, 2)), jnp.float32),
        "line_limit": jnp.clip(jnp.exp(math.log(2.0) - 2.3025851 * jax.random.uniform(keys[10], (L,), jnp.float32) ** level_of(keys[10], (L,), ((0, 2),), -0.2, 0.2)), 0.2, 2.0),
        "line_dual": centred(keys[11], (HOURS, L), 0.5, 3.0, ((0, 128), (1, 2)), jnp.float32),
        "ramp_dual": centred(keys[12], (HOURS, G), 0.5, 3.0, ((0, 128), (1, 2)), jnp.float32),
        "balance_dual": centred(keys[13], (HOURS,), 1.0, 5.0, ((0, 128),), jnp.float32),
    }


TAU = 0.35
SIGMA = 0.35


def reference(dispatch, cost, p_low, p_high, ramp_limit, p_init, demand, bus_of, ptdf, line_base, line_limit, line_dual, ramp_dual, balance_dual):
    factors = jnp.take(ptdf, bus_of.astype(jnp.int32), axis=1).astype(jnp.float32)
    weight_bal = float(G) ** -0.5
    hours = dispatch.shape[0]
    cells = float(hours) * float(G)
    state_x = dispatch
    duals = line_dual
    ramp_mult = ramp_dual
    balance = balance_dual
    records = []
    for step in range(ITERS):
        rounded = duals.astype(jnp.bfloat16).astype(jnp.float32)
        pulled = jnp.dot(rounded, factors, precision=lax.Precision.HIGHEST)
        after = jnp.concatenate([ramp_mult[1:], jnp.zeros((1, G), jnp.float32)], 0)
        grad = cost[None, :] + weight_bal * balance[:, None] + pulled + ramp_mult - after
        x_new = jnp.clip(state_x - TAU * grad, p_low[None, :], p_high[None, :])
        xbar = 2.0 * x_new - state_x
        xbar_round = xbar.astype(jnp.bfloat16).astype(jnp.float32)
        flows = jnp.dot(xbar_round, factors.T, precision=lax.Precision.HIGHEST)
        totals = weight_bal * jnp.sum(xbar, axis=1)
        balance_new = balance + SIGMA * (totals - demand)
        moved = duals + SIGMA * flows
        low = line_base - line_limit[None, :]
        high = line_base + line_limit[None, :]
        duals_new = moved - SIGMA * jnp.clip(moved / SIGMA, low, high)
        before = jnp.concatenate([p_init[None, :], xbar[:-1]], 0)
        shifted = ramp_mult + SIGMA * (xbar - before)
        ramp_new = shifted - SIGMA * jnp.clip(shifted / SIGMA, -ramp_limit[None, :], ramp_limit[None, :])
        primal = jnp.sum((x_new - state_x) * (x_new - state_x)) / (TAU * cells)
        dual = (jnp.sum((duals_new - duals) * (duals_new - duals)) + jnp.sum((ramp_new - ramp_mult) * (ramp_new - ramp_mult)) + jnp.sum((balance_new - balance) * (balance_new - balance))) / (SIGMA * cells)
        records.append(jnp.stack([primal, dual]))
        state_x, duals, ramp_mult, balance = x_new, duals_new, ramp_new, balance_new
    return state_x, duals, ramp_mult, balance, jnp.stack(records)
```

```python
import functools
import math

import jax
import jax.numpy as jnp
from jax import lax
from jax.experimental import pallas as pl
from jax.experimental.pallas import tpu as pltpu
from jax.sharding import PartitionSpec as P

TAU = 0.35
SIGMA = 0.35
ITERS = 2
PLANE = 16
MESH = pl.DeviceIdType.MESH
BF16 = jnp.bfloat16
F32 = jnp.float32


def kernel(
    cfg,
    bus, x_h, cost_h, lo_h, hi_h, ramp_h, pinit_h, dem_h, ptdf_h, base_h, lim_h, y_h, mu_h, lam_h,
    xo_h, yo_h, muo_h, lam_o, mov_o,
    ptdf, table, stage, fac, xv, muv, xbv, xbb, yv, basev, flow_own, yb, fsend, frecv,
    cost, lo, hi, ramp, pinit, lim, dem, lam, mu_next, xb_prev, xb_next,
    acc_p, acc_d, acc_t, msg, ar_a, ar_b,
    load_sem, ptdf_sem, out_sem, yb_send, yb_recv, f_send, f_recv, row_send, row_recv, ar_send, ar_recv,
):
    ntm, plane, gl_total, hours = cfg
    rows, gl = x_h.shape
    lines, buses = ptdf_h.shape
    half = lines // 2
    nz = ntm // plane
    w = 1.0 / math.sqrt(gl_total)
    cells = float(hours) * float(gl_total)
    tm = lax.axis_index("tm")
    gen = lax.axis_index("gen")
    other = 1 - gen
    partner = (tm, other)
    nxt = (lax.rem(tm + 1, ntm), gen)
    prv = (lax.rem(tm + ntm - 1, ntm), gen)
    zz = tm // plane
    in_plane = lax.rem(tm, plane)
    n_a = 2 * plane
    mine_a = in_plane * 2 + gen

    def peer_a(d):
        q = lax.rem(mine_a + d, n_a)
        return (zz * plane + q // 2, lax.rem(q, 2))

    def peer_b(d):
        return (lax.rem(zz + d, nz) * plane + in_plane, gen)

    nblk = buses // 256
    ptdf_copies = []
    for c in range(nblk):
        cp = pltpu.make_async_copy(
            ptdf_h.at[:, pl.ds(c * 256, 256)], ptdf.at[:, pl.ds(c * 256, 256)], ptdf_sem.at[c]
        )
        cp.start()
        ptdf_copies.append(cp)
    loads = [
        pltpu.make_async_copy(s, d, load_sem.at[i])
        for i, (s, d) in enumerate(
            [
                (y_h, yv), (mu_h, muv.at[pl.ds(0, rows)]), (x_h, xv), (base_h, basev), (cost_h, cost),
                (lo_h, lo), (hi_h, hi), (ramp_h, ramp), (pinit_h, pinit), (lim_h, lim), (dem_h, dem),
                (lam_h, lam),
            ]
        )
    ]
    for cp in loads:
        cp.start()

    barrier = pltpu.get_barrier_semaphore()

    def greet(dev):
        pl.semaphore_signal(barrier, inc=1, device_id=dev, device_id_type=MESH)

    greet(nxt)
    greet(prv)

    @pl.loop(1, n_a)
    def _(d):
        greet(peer_a(d))

    @pl.loop(1, nz)
    def _(d):
        greet(peer_b(d))

    nlb = lines // 128
    eye = (
        lax.broadcasted_iota(jnp.int32, (256, 256), 0)
        == lax.broadcasted_iota(jnp.int32, (256, 256), 1)
    ).astype(BF16)
    for c in range(nblk):
        ptdf_copies[c].wait()
        turned = lax.dot_general(
            eye, ptdf[:, c * 256 : (c + 1) * 256], (((1,), (1,)), ((), ())),
            preferred_element_type=F32,
        )
        for j in range(nlb):
            table[pl.ds(c * 256, 256), j, :] = turned[:, j * 128 : (j + 1) * 128]

    for cp in loads:
        cp.wait()
    yb[0, gen] = yv[...].astype(BF16)
    pl.semaphore_wait(barrier, n_a - 1 + nz - 1 + 2)

    def send_yb(it):
        return pltpu.make_async_remote_copy(
            yb.at[it, gen], yb.at[it, gen], yb_send.at[it], yb_recv.at[it],
            device_id=partner, device_id_type=MESH,
        )

    def send_row(k, src, dst, dev):
        return pltpu.make_async_remote_copy(
            src, dst, row_send.at[k], row_recv.at[k], device_id=dev, device_id_type=MESH
        )

    yb_copy = send_yb(0)
    yb_copy.start()
    mu_copy = send_row(0, muv.at[pl.ds(0, 1)], mu_next, prv)
    mu_copy.start()

    group = 16

    @pl.loop(0, gl // (2 * group))
    def _(i):
        for s in range(2):
            g0 = pl.multiple_of((i * 2 + s) * group, group)
            for k in range(group):
                stage[pl.ds((s * group + k) * nlb, nlb), :] = table[bus[g0 + k]]
            for j in range(nlb):
                got = stage[pl.ds(s * group * nlb + j, group, stride=nlb), :]
                fac[j // (nlb // 2), pl.ds(g0, group), pl.ds((j % (nlb // 2)) * 128, 128)] = got.astype(BF16)

    eye_r = lax.broadcasted_iota(jnp.int32, (rows, rows), 0) == lax.broadcasted_iota(
        jnp.int32, (rows, rows), 1
    )

    def to_column(row):
        return jnp.sum(jnp.where(eye_r, jnp.broadcast_to(row, (rows, rows)), 0.0), axis=1, keepdims=True)

    def to_row(col):
        return jnp.sum(jnp.where(eye_r, jnp.broadcast_to(col, (rows, rows)), 0.0), axis=0, keepdims=True)

    last = tm == ntm - 1
    first = tm == 0
    lam_col = to_column(lam[...])
    dem_col = to_column(dem[...])
    yb_copy.wait()
    mu_copy.wait()
    muv[pl.ds(rows, 1), :] = jnp.where(last, 0.0, mu_next[...])

    gc = 512
    sums = []
    outs = []
    for it in range(ITERS):
        acc_p[...] = jnp.zeros_like(acc_p)
        acc_d[...] = jnp.zeros_like(acc_d)
        acc_t[...] = jnp.zeros_like(acc_t)
        wlam = w * lam_col

        @pl.loop(0, gl // gc)
        def _(c):
            sl = pl.ds(pl.multiple_of(c * gc, gc), gc)
            pulled = lax.dot_general(
                yb[it, 0], fac[0, sl, :], (((1,), (1,)), ((), ())), preferred_element_type=F32
            ) + lax.dot_general(
                yb[it, 1], fac[1, sl, :], (((1,), (1,)), ((), ())), preferred_element_type=F32
            )
            xc = xv[:, sl]
            grad = cost[:, sl] + wlam + pulled + muv[pl.ds(0, rows), sl] - muv[pl.ds(1, rows), sl]
            xn = jnp.clip(xc - TAU * grad, lo[:, sl], hi[:, sl])
            xb = 2.0 * xn - xc
            d = xn - xc
            d2 = d * d
            xv[:, sl] = xn
            xbv[pl.ds(8, rows), sl] = xb
            xbb[:, sl] = xb.astype(BF16)
            acc_p[...] += sum(d2[:, k * 128 : (k + 1) * 128] for k in range(gc // 128))
            acc_t[...] += sum(xb[:, k * 128 : (k + 1) * 128] for k in range(gc // 128))

        rows_out = [send_row(1 + 2 * it, xbv.at[pl.ds(8 + rows - 1, 1)], xb_prev.at[it], nxt)]
        if it < ITERS - 1:
            rows_out.append(send_row(2 + 2 * it, xbv.at[pl.ds(8, 1)], xb_next, prv))
        for cp in rows_out:
            cp.start()
        if it == ITERS - 1:
            cp = pltpu.make_async_copy(xv, xo_h, out_sem.at[0])
            cp.start()
            outs.append(cp)

        tot_col = w * jnp.sum(acc_t[...], axis=1, keepdims=True)
        fsend[it, pl.ds(0, rows), :] = jnp.dot(xbb[...], fac[other], preferred_element_type=F32)
        fsend[it, pl.ds(rows, 1), pl.ds(0, rows)] = to_row(tot_col)
        f_copy = pltpu.make_async_remote_copy(
            fsend.at[it], frecv.at[it], f_send.at[it], f_recv.at[it],
            device_id=partner, device_id_type=MESH,
        )
        f_copy.start()
        flow_own[...] = jnp.dot(xbb[...], fac[gen], preferred_element_type=F32)

        for cp in rows_out:
            cp.wait()
        xbv[pl.ds(7, 1), :] = jnp.where(first, pinit[...], xb_prev[it])
        if it < ITERS - 1:
            m_n = muv[pl.ds(rows, 1), :]
            u_n = m_n + SIGMA * (xb_next[...] - xbv[pl.ds(8 + rows - 1, 1), :])
            mn_n = u_n - jnp.clip(u_n, -SIGMA * ramp[...], SIGMA * ramp[...])
            muv[pl.ds(rows, 1), :] = jnp.where(last, 0.0, mn_n)

        @pl.loop(0, gl // gc)
        def _(c):
            sl = pl.ds(pl.multiple_of(c * gc, gc), gc)
            m = muv[pl.ds(0, rows), sl]
            u = m + SIGMA * (xbv[pl.ds(8, rows), sl] - xbv[pl.ds(7, rows), sl])
            r = SIGMA * ramp[:, sl]
            mn = u - jnp.clip(u, -r, r)
            muv[pl.ds(0, rows), sl] = mn
            d = mn - m
            d2 = d * d
            acc_d[...] += sum(d2[:, k * 128 : (k + 1) * 128] for k in range(gc // 128))

        if it == ITERS - 1:
            cp = pltpu.make_async_copy(muv.at[pl.ds(0, rows)], muo_h, out_sem.at[1])
            cp.start()
            outs.append(cp)

        f_copy.wait()
        yo = yv[...]
        v = yo + SIGMA * (flow_own[...] + frecv[it, pl.ds(0, rows), :])
        bv = basev[...]
        lv = lim[...]
        yn = v - jnp.clip(v, SIGMA * (bv - lv), SIGMA * (bv + lv))
        yv[...] = yn
        if it < ITERS - 1:
            yb[it + 1, gen] = yn.astype(BF16)
            yb_copy = send_yb(it + 1)
            yb_copy.start()
        else:
            cp = pltpu.make_async_copy(yv, yo_h, out_sem.at[2])
            cp.start()
            outs.append(cp)
        dy = yn - yo
        dy2 = dy * dy
        acc_d[...] += sum(dy2[:, k * 128 : (k + 1) * 128] for k in range(half // 128))
        totals = tot_col + to_column(frecv[it, pl.ds(rows, 1), pl.ds(0, rows)])
        lam_new = lam_col + SIGMA * (totals - dem_col)
        dl = lam_new - lam_col
        lam_col = lam_new
        primal = jnp.sum(acc_p[...], keepdims=True) / (TAU * cells)
        dual = (
            jnp.sum(acc_d[...], keepdims=True)
            + jnp.where(gen == 0, jnp.sum(dl * dl, keepdims=True), 0.0)
        ) / (SIGMA * cells)
        sums += [primal, dual]
        if it < ITERS - 1:
            yb_copy.wait()

    lane = lax.broadcasted_iota(jnp.int32, (1, 128), 1)
    packed = jnp.zeros((1, 128), F32)
    for k, s in enumerate(sums):
        packed = jnp.where(lane == k, s, packed)

    def all_sum(value, buf, k, n, mine, peer):
        msg[k] = value
        buf[mine] = value

        @pl.loop(1, n)
        def _(d):
            pltpu.make_async_remote_copy(
                msg.at[k], buf.at[mine], ar_send.at[k], ar_recv.at[k],
                device_id=peer(d), device_id_type=MESH,
            ).start()

        several = buf.at[pl.ds(0, n - 1)]
        pltpu.make_async_copy(several, several, ar_send.at[k]).wait()
        pltpu.make_async_copy(several, several, ar_recv.at[k]).wait()
        return jnp.sum(buf[...], axis=0)

    total = all_sum(packed, ar_a, 0, n_a, mine_a, peer_a)
    total = all_sum(total, ar_b, 1, nz, zz, peer_b)
    place = 2 * lax.broadcasted_iota(jnp.int32, (ITERS, 2), 0) + lax.broadcasted_iota(
        jnp.int32, (ITERS, 2), 1
    )
    result = jnp.zeros((ITERS, 2), F32)
    for k in range(2 * ITERS):
        one = jnp.sum(jnp.where(lane == k, total, 0.0), axis=1, keepdims=True)
        result = jnp.where(place == k, one, result)
    mov_o[...] = result
    lam_o[...] = to_row(lam_col)
    for cp in outs:
        cp.wait()


def on_device(ntm, plane, hours, gl_total,
              dispatch, cost, p_low, p_high, ramp_limit, p_init, demand, bus_of, ptdf, line_base,
              line_limit, line_dual, ramp_dual, balance_dual):
    rows, gl = dispatch.shape
    lines, buses = ptdf.shape
    half = lines // 2
    n_a = 2 * plane
    nz = ntm // plane
    row = lambda a: a.reshape(1, -1)
    any_ = pl.BlockSpec(memory_space=pl.ANY)
    vmem = pl.BlockSpec(memory_space=pltpu.VMEM)
    smem = pl.BlockSpec(memory_space=pltpu.SMEM)
    V = pltpu.VMEM
    S = pltpu.SemaphoreType.DMA
    x, y, mu, lam, mov = pl.pallas_call(
        functools.partial(kernel, (ntm, plane, gl_total, hours)),
        name="dispatch_step",
        out_shape=(
            jax.ShapeDtypeStruct((rows, gl), F32),
            jax.ShapeDtypeStruct((rows, half), F32),
            jax.ShapeDtypeStruct((rows, gl), F32),
            jax.ShapeDtypeStruct((1, rows), F32),
            jax.ShapeDtypeStruct((ITERS, 2), F32),
        ),
        in_specs=[smem] + [any_] * 13,
        out_specs=(any_, any_, any_, vmem, vmem),
        scratch_shapes=[
            V((lines, buses), BF16),
            V((buses, lines // 128, 128), F32),
            V((32 * (lines // 128), 128), F32),
            V((2, gl, half), BF16),
            V((rows, gl), F32),
            V((rows + 8, gl), F32),
            V((rows + 8, gl), F32),
            V((rows, gl), BF16),
            V((rows, half), F32),
            V((rows, half), F32),
            V((rows, half), F32),
            V((ITERS, 2, rows, half), BF16),
            V((ITERS, rows + 8, half), F32),
            V((ITERS, rows + 8, half), F32),
            V((1, gl), F32), V((1, gl), F32), V((1, gl), F32), V((1, gl), F32), V((1, gl), F32),
            V((1, half), F32), V((1, rows), F32), V((1, rows), F32),
            V((1, gl), F32), V((ITERS, 1, gl), F32), V((1, gl), F32),
            V((rows, 128), F32), V((rows, 128), F32), V((rows, 128), F32),
            V((2, 1, 128), F32), V((n_a, 1, 128), F32), V((nz, 1, 128), F32),
            S((12,)), S((buses // 256,)), S((3,)), S((ITERS,)), S((ITERS,)), S((ITERS,)), S((ITERS,)),
            S((2 * ITERS,)), S((2 * ITERS,)), S((2,)), S((2,)),
        ],
        compiler_params=pltpu.CompilerParams(
            collective_id=0, has_side_effects=True, vmem_limit_bytes=48 * 1024 * 1024
        ),
    )(
        bus_of, dispatch, row(cost), row(p_low), row(p_high), row(ramp_limit), row(p_init), row(demand),
        ptdf, line_base, row(line_limit), line_dual, ramp_dual, row(balance_dual),
    )
    return x, y, mu, lam.reshape(-1), mov


def solution(mesh):
    ntm = mesh.shape["tm"]
    plane = min(PLANE, ntm)

    def body(*args):
        return on_device(ntm, plane, args[0].shape[0] * ntm, args[0].shape[1] * mesh.shape["gen"], *args)

    in_specs = (
        P("tm", "gen"), P("gen"), P("gen"), P("gen"), P("gen"), P("gen"), P("tm"), P("gen"), P(),
        P("tm", "gen"), P("gen"), P("tm", "gen"), P("tm", "gen"), P("tm"),
    )
    out_specs = (P("tm", "gen"), P("tm", "gen"), P("tm", "gen"), P("tm"), P())
    return jax.shard_map(body, mesh=mesh, in_specs=in_specs, out_specs=out_specs, check_vma=False)
```

```python
import functools
import math

import jax
import jax.numpy as jnp
from jax import lax
from jax.experimental import pallas as pl
from jax.experimental.pallas import tpu as pltpu
from jax.sharding import PartitionSpec as P

TAU = 0.35
SIGMA = 0.35
ITERS = 2
PLANE = 16
MESH = pl.DeviceIdType.MESH
BF16 = jnp.bfloat16
F32 = jnp.float32


def kernel(
    cfg,
    bus_h, x_h, cost_h, lo_h, hi_h, ramp_h, pinit_h, dem_h, ptdf_h, base_h, lim_h, y_h, mu_h, lam_h,
    xo_h, yo_h, muo_h, lam_o, mov_o,
    ptdf, table, stage, fac, xv, muv, xbv, xbb, yv, basev, flow_own, yb, fsend, frecv,
    bus, cost, lo, hi, ramp, pinit, lim, dem, lam, mu_next, xb_prev, xb_next,
    acc_p, acc_d, acc_t, msg, ar_a, ar_b,
    load_sem, ptdf_sem, out_sem, yb_send, yb_recv, f_send, f_recv, row_send, row_recv, ar_send, ar_recv,
):
    ntm, plane, gl_total, hours = cfg
    rows, gl = x_h.shape
    lines, buses = ptdf_h.shape
    half = lines // 2
    nz = ntm // plane
    w = 1.0 / math.sqrt(gl_total)
    cells = float(hours) * float(gl_total)
    tm = lax.axis_index("tm")
    gen = lax.axis_index("gen")
    other = 1 - gen
    partner = (tm, other)
    nxt = (lax.rem(tm + 1, ntm), gen)
    prv = (lax.rem(tm + ntm - 1, ntm), gen)
    zz = tm // plane
    in_plane = lax.rem(tm, plane)
    n_a = 2 * plane
    mine_a = in_plane * 2 + gen

    def peer_a(d):
        q = lax.rem(mine_a + d, n_a)
        return (zz * plane + q // 2, lax.rem(q, 2))

    def peer_b(d):
        return (lax.rem(zz + d, nz) * plane + in_plane, gen)

    nblk = buses // 256
    per_load = nblk // 2
    ptdf_copies = []
    for c in range(2):
        part = pl.ds(c * per_load * 256, per_load * 256)
        cp = pltpu.make_async_copy(ptdf_h.at[:, part], ptdf.at[:, part], ptdf_sem.at[c])
        cp.start()
        ptdf_copies.append(cp)
    loads = [
        pltpu.make_async_copy(s, d, load_sem.at[i])
        for i, (s, d) in enumerate(
            [
                (y_h, yv), (mu_h, muv.at[pl.ds(0, rows)]), (x_h, xv), (base_h, basev), (cost_h, cost),
                (lo_h, lo), (hi_h, hi), (ramp_h, ramp), (pinit_h, pinit), (lim_h, lim), (dem_h, dem),
                (lam_h, lam), (bus_h, bus),
            ]
        )
    ]
    for cp in loads:
        cp.start()

    barrier = pltpu.get_barrier_semaphore()

    def greet(dev):
        pl.semaphore_signal(barrier, inc=1, device_id=dev, device_id_type=MESH)

    greet(nxt)
    greet(prv)

    @pl.loop(1, n_a)
    def _(d):
        greet(peer_a(d))

    @pl.loop(1, nz)
    def _(d):
        greet(peer_b(d))

    nlb = lines // 128
    flat = table.reshape(buses * nlb, 128)
    eye = (
        lax.broadcasted_iota(jnp.int32, (256, 256), 0)
        == lax.broadcasted_iota(jnp.int32, (256, 256), 1)
    ).astype(BF16)
    for c in range(nblk):
        if c % per_load == 0:
            ptdf_copies[c // per_load].wait()
        turned = lax.dot_general(
            eye, ptdf[:, c * 256 : (c + 1) * 256], (((1,), (1,)), ((), ())),
            preferred_element_type=F32,
        )
        for j in range(nlb):
            flat[pl.ds(c * 256 * nlb + j, 256, stride=nlb), :] = turned[:, j * 128 : (j + 1) * 128]

    for cp in loads:
        cp.wait()
    yb[0, gen] = yv[...].astype(BF16)
    pl.semaphore_wait(barrier, n_a - 1 + nz - 1 + 2)

    def send_yb(it):
        return pltpu.make_async_remote_copy(
            yb.at[it, gen], yb.at[it, gen], yb_send.at[it], yb_recv.at[it],
            device_id=partner, device_id_type=MESH,
        )

    def send_row(k, src, dst, dev):
        return pltpu.make_async_remote_copy(
            src, dst, row_send.at[k], row_recv.at[k], device_id=dev, device_id_type=MESH
        )

    yb_copy = send_yb(0)
    yb_copy.start()
    mu_copy = send_row(0, muv.at[pl.ds(0, 1)], mu_next, prv)
    mu_copy.start()

    group = 16
    n_group = 128 // group

    @pl.loop(0, gl // 128)
    def _(i):
        def fetch(s, k):
            stage[pl.ds((s * group + k) * nlb, nlb), :] = table[bus[i, s * group + k]]

        def pack(s, j):
            g0 = pl.multiple_of(i * 128 + s * group, group)
            got = stage[pl.ds(s * group * nlb + j, group, stride=nlb), :]
            fac[j // (nlb // 2), pl.ds(g0, group), pl.ds((j % (nlb // 2)) * 128, 128)] = got.astype(BF16)

        for k in range(group):
            fetch(0, k)
        for s in range(n_group):
            per = group // nlb
            for j in range(nlb):
                if s + 1 < n_group:
                    for k in range(per):
                        fetch(s + 1, j * per + k)
                pack(s, j)

    eye_r = lax.broadcasted_iota(jnp.int32, (rows, rows), 0) == lax.broadcasted_iota(
        jnp.int32, (rows, rows), 1
    )

    def to_column(row):
        return jnp.sum(jnp.where(eye_r, jnp.broadcast_to(row, (rows, rows)), 0.0), axis=1, keepdims=True)

    def to_row(col):
        return jnp.sum(jnp.where(eye_r, jnp.broadcast_to(col, (rows, rows)), 0.0), axis=0, keepdims=True)

    last = tm == ntm - 1
    first = tm == 0
    lam_col = to_column(lam[...])
    dem_col = to_column(dem[...])
    yb_copy.wait()
    mu_copy.wait()
    muv[pl.ds(rows, 1), :] = jnp.where(last, 0.0, mu_next[...])

    gc = 512
    sums = []
    outs = []
    for it in range(ITERS):
        acc_p[...] = jnp.zeros_like(acc_p)
        acc_d[...] = jnp.zeros_like(acc_d)
        acc_t[...] = jnp.zeros_like(acc_t)
        wlam = w * lam_col

        @pl.loop(0, gl // gc)
        def _(c):
            sl = pl.ds(pl.multiple_of(c * gc, gc), gc)
            pulled = lax.dot_general(
                yb[it, 0], fac[0, sl, :], (((1,), (1,)), ((), ())), preferred_element_type=F32
            ) + lax.dot_general(
                yb[it, 1], fac[1, sl, :], (((1,), (1,)), ((), ())), preferred_element_type=F32
            )
            xc = xv[:, sl]
            grad = cost[:, sl] + wlam + pulled + muv[pl.ds(0, rows), sl] - muv[pl.ds(1, rows), sl]
            xn = jnp.clip(xc - TAU * grad, lo[:, sl], hi[:, sl])
            xb = 2.0 * xn - xc
            d = xn - xc
            d2 = d * d
            xv[:, sl] = xn
            xbv[pl.ds(8, rows), sl] = xb
            xbb[:, sl] = xb.astype(BF16)
            acc_p[...] += sum(d2[:, k * 128 : (k + 1) * 128] for k in range(gc // 128))
            acc_t[...] += sum(xb[:, k * 128 : (k + 1) * 128] for k in range(gc // 128))

        rows_out = [send_row(1 + 2 * it, xbv.at[pl.ds(8 + rows - 1, 1)], xb_prev.at[it], nxt)]
        if it < ITERS - 1:
            rows_out.append(send_row(2 + 2 * it, xbv.at[pl.ds(8, 1)], xb_next, prv))
        for cp in rows_out:
            cp.start()
        if it == ITERS - 1:
            cp = pltpu.make_async_copy(xv, xo_h, out_sem.at[0])
            cp.start()
            outs.append(cp)

        tot_col = w * jnp.sum(acc_t[...], axis=1, keepdims=True)
        fsend[it, pl.ds(0, rows), :] = jnp.dot(xbb[...], fac[other], preferred_element_type=F32)
        fsend[it, pl.ds(rows, 1), pl.ds(0, rows)] = to_row(tot_col)
        f_copy = pltpu.make_async_remote_copy(
            fsend.at[it], frecv.at[it], f_send.at[it], f_recv.at[it],
            device_id=partner, device_id_type=MESH,
        )
        f_copy.start()
        flow_own[...] = jnp.dot(xbb[...], fac[gen], preferred_element_type=F32)

        for cp in rows_out:
            cp.wait()
        xbv[pl.ds(7, 1), :] = jnp.where(first, pinit[...], xb_prev[it])
        if it < ITERS - 1:
            m_n = muv[pl.ds(rows, 1), :]
            u_n = m_n + SIGMA * (xb_next[...] - xbv[pl.ds(8 + rows - 1, 1), :])
            mn_n = u_n - jnp.clip(u_n, -SIGMA * ramp[...], SIGMA * ramp[...])
            muv[pl.ds(rows, 1), :] = jnp.where(last, 0.0, mn_n)

        @pl.loop(0, gl // gc)
        def _(c):
            sl = pl.ds(pl.multiple_of(c * gc, gc), gc)
            m = muv[pl.ds(0, rows), sl]
            u = m + SIGMA * (xbv[pl.ds(8, rows), sl] - xbv[pl.ds(7, rows), sl])
            r = SIGMA * ramp[:, sl]
            mn = u - jnp.clip(u, -r, r)
            muv[pl.ds(0, rows), sl] = mn
            d = mn - m
            d2 = d * d
            acc_d[...] += sum(d2[:, k * 128 : (k + 1) * 128] for k in range(gc // 128))

        if it == ITERS - 1:
            cp = pltpu.make_async_copy(muv.at[pl.ds(0, rows)], muo_h, out_sem.at[1])
            cp.start()
            outs.append(cp)

        f_copy.wait()
        yo = yv[...]
        v = yo + SIGMA * (flow_own[...] + frecv[it, pl.ds(0, rows), :])
        bv = basev[...]
        lv = lim[...]
        yn = v - jnp.clip(v, SIGMA * (bv - lv), SIGMA * (bv + lv))
        yv[...] = yn
        if it < ITERS - 1:
            yb[it + 1, gen] = yn.astype(BF16)
            yb_copy = send_yb(it + 1)
            yb_copy.start()
        else:
            cp = pltpu.make_async_copy(yv, yo_h, out_sem.at[2])
            cp.start()
            outs.append(cp)
        dy = yn - yo
        dy2 = dy * dy
        acc_d[...] += sum(dy2[:, k * 128 : (k + 1) * 128] for k in range(half // 128))
        totals = tot_col + to_column(frecv[it, pl.ds(rows, 1), pl.ds(0, rows)])
        lam_new = lam_col + SIGMA * (totals - dem_col)
        dl = lam_new - lam_col
        lam_col = lam_new
        primal = jnp.sum(acc_p[...], keepdims=True) / (TAU * cells)
        dual = (
            jnp.sum(acc_d[...], keepdims=True)
            + jnp.where(gen == 0, jnp.sum(dl * dl, keepdims=True), 0.0)
        ) / (SIGMA * cells)
        sums += [primal, dual]
        if it < ITERS - 1:
            yb_copy.wait()

    lane = lax.broadcasted_iota(jnp.int32, (1, 128), 1)
    packed = jnp.zeros((1, 128), F32)
    for k, s in enumerate(sums):
        packed = jnp.where(lane == k, s, packed)

    def all_sum(value, buf, k, n, mine, peer):
        msg[k] = value
        buf[mine] = value

        @pl.loop(1, n)
        def _(d):
            pltpu.make_async_remote_copy(
                msg.at[k], buf.at[mine], ar_send.at[k], ar_recv.at[k],
                device_id=peer(d), device_id_type=MESH,
            ).start()

        several = buf.at[pl.ds(0, n - 1)]
        pltpu.make_async_copy(several, several, ar_send.at[k]).wait()
        pltpu.make_async_copy(several, several, ar_recv.at[k]).wait()
        return jnp.sum(buf[...], axis=0)

    total = all_sum(packed, ar_a, 0, n_a, mine_a, peer_a)
    total = all_sum(total, ar_b, 1, nz, zz, peer_b)
    place = 2 * lax.broadcasted_iota(jnp.int32, (ITERS, 2), 0) + lax.broadcasted_iota(
        jnp.int32, (ITERS, 2), 1
    )
    result = jnp.zeros((ITERS, 2), F32)
    for k in range(2 * ITERS):
        one = jnp.sum(jnp.where(lane == k, total, 0.0), axis=1, keepdims=True)
        result = jnp.where(place == k, one, result)
    mov_o[...] = result
    lam_o[...] = to_row(lam_col)
    for cp in outs:
        cp.wait()


def on_device(ntm, plane, hours, gl_total,
              dispatch, cost, p_low, p_high, ramp_limit, p_init, demand, bus_of, ptdf, line_base,
              line_limit, line_dual, ramp_dual, balance_dual):
    rows, gl = dispatch.shape
    lines, buses = ptdf.shape
    half = lines // 2
    n_a = 2 * plane
    nz = ntm // plane
    row = lambda a: a.reshape(1, -1)
    any_ = pl.BlockSpec(memory_space=pltpu.HBM)
    vmem = pl.BlockSpec(memory_space=pltpu.VMEM)
    V = pltpu.VMEM
    S = pltpu.SemaphoreType.DMA
    x, y, mu, lam, mov = pl.pallas_call(
        functools.partial(kernel, (ntm, plane, gl_total, hours)),
        name="dispatch_step",
        out_shape=(
            jax.ShapeDtypeStruct((rows, gl), F32),
            jax.ShapeDtypeStruct((rows, half), F32),
            jax.ShapeDtypeStruct((rows, gl), F32),
            jax.ShapeDtypeStruct((1, rows), F32),
            jax.ShapeDtypeStruct((ITERS, 2), F32),
        ),
        in_specs=[any_] * 14,
        out_specs=(any_, any_, any_, vmem, vmem),
        scratch_shapes=[
            V((lines, buses), BF16),
            V((buses, lines // 128, 128), F32),
            V((128 * (lines // 128), 128), F32),
            V((2, gl, half), BF16),
            V((rows, gl), F32),
            V((rows + 8, gl), F32),
            V((rows + 8, gl), F32),
            V((rows, gl), BF16),
            V((rows, half), F32),
            V((rows, half), F32),
            V((rows, half), F32),
            V((ITERS, 2, rows, half), BF16),
            V((ITERS, rows + 8, half), F32),
            V((ITERS, rows + 8, half), F32),
            pltpu.SMEM((gl // 128, 128), jnp.int32),
            V((1, gl), F32), V((1, gl), F32), V((1, gl), F32), V((1, gl), F32), V((1, gl), F32),
            V((1, half), F32), V((1, rows), F32), V((1, rows), F32),
            V((1, gl), F32), V((ITERS, 1, gl), F32), V((1, gl), F32),
            V((rows, 128), F32), V((rows, 128), F32), V((rows, 128), F32),
            V((2, 1, 128), F32), V((n_a, 1, 128), F32), V((nz, 1, 128), F32),
            S((13,)), S((2,)), S((3,)), S((ITERS,)), S((ITERS,)), S((ITERS,)), S((ITERS,)),
            S((2 * ITERS,)), S((2 * ITERS,)), S((2,)), S((2,)),
        ],
        compiler_params=pltpu.CompilerParams(
            collective_id=0, has_side_effects=True, vmem_limit_bytes=60 * 1024 * 1024
        ),
    )(
        bus_of.reshape(-1, 128), dispatch, row(cost), row(p_low), row(p_high), row(ramp_limit), row(p_init), row(demand),
        ptdf, line_base, row(line_limit), line_dual, ramp_dual, row(balance_dual),
    )
    return x, y, mu, lam.reshape(-1), mov


def solution(mesh):
    ntm = mesh.shape["tm"]
    plane = min(PLANE, ntm)

    def body(*args):
        return on_device(ntm, plane, args[0].shape[0] * ntm, args[0].shape[1] * mesh.shape["gen"], *args)

    in_specs = (
        P("tm", "gen"), P("gen"), P("gen"), P("gen"), P("gen"), P("gen"), P("tm"), P("gen"), P(),
        P("tm", "gen"), P("gen"), P("tm", "gen"), P("tm", "gen"), P("tm"),
    )
    out_specs = (P("tm", "gen"), P("tm", "gen"), P("tm", "gen"), P("tm"), P())
    return jax.shard_map(body, mesh=mesh, in_specs=in_specs, out_specs=out_specs, check_vma=False)
```

```python
import functools
import math

import jax
import jax.numpy as jnp
from jax import lax
from jax.experimental import pallas as pl
from jax.experimental.pallas import tpu as pltpu
from jax.sharding import PartitionSpec as P

TAU = 0.35
SIGMA = 0.35
ITERS = 2
PLANE = 16
MESH = pl.DeviceIdType.MESH
BF16 = jnp.bfloat16
F32 = jnp.float32


def kernel(
    cfg,
    bus_h, x_h, cost_h, lo_h, hi_h, ramp_h, pinit_h, dem_h, ptdf_h, base_h, lim_h, y_h, mu_h, lam_h,
    xv, yo, muo, lam_o, mov_o,
    ptdf, table, stage, fac, muv, xbv, xbb, yv, yt, bt, flow, yb, ybs, frecv,
    bus, cost, lo, hi, ramp, pinit, lim, lim_x, dem, lam, mu_next, xb_prev, xb_next, tot, tot_x,
    acc_p, acc_d, acc_t, msg, ar_a, ar_b,
    load_sem, ptdf_sem, yb_send, yb_recv, init_send, init_recv, f_send, f_recv, t_send, t_recv,
    ys_send, ys_recv, yr_send, yr_recv, row_send, row_recv, ar_send, ar_recv,
):
    ntm, plane, gl_total, hours = cfg
    rows, gl = x_h.shape
    lines, buses = ptdf_h.shape
    half = lines // 2
    nz = ntm // plane
    w = 1.0 / math.sqrt(gl_total)
    cells = float(hours) * float(gl_total)
    tm = lax.axis_index("tm")
    gen = lax.axis_index("gen")
    other = 1 - gen
    partner = (tm, other)
    nxt = (lax.rem(tm + 1, ntm), gen)
    prv = (lax.rem(tm + ntm - 1, ntm), gen)
    twin = tm + 2 - 4 * lax.rem(tm // 2, 2)
    top = pl.ds(0, rows // 2)
    low = pl.ds(rows // 2, rows // 2)
    zz = tm // plane
    in_plane = lax.rem(tm, plane)
    n_a = 2 * plane
    mine_a = in_plane * 2 + gen

    def peer_a(d):
        q = lax.rem(mine_a + d, n_a)
        return (zz * plane + q // 2, lax.rem(q, 2))

    def peer_b(d):
        return (lax.rem(zz + d, nz) * plane + in_plane, gen)

    nblk = buses // 256
    per_load = nblk // 2
    ptdf_copies = []
    for c in range(2):
        part = pl.ds(c * per_load * 256, per_load * 256)
        cp = pltpu.make_async_copy(ptdf_h.at[:, part], ptdf.at[:, part], ptdf_sem.at[c])
        cp.start()
        ptdf_copies.append(cp)
    loads = [
        pltpu.make_async_copy(s, d, load_sem.at[i])
        for i, (s, d) in enumerate(
            [
                (y_h, yv), (mu_h, muv.at[pl.ds(0, rows)]), (x_h, xv), (cost_h, cost),
                (lo_h, lo), (hi_h, hi), (ramp_h, ramp), (pinit_h, pinit), (lim_h, lim), (dem_h, dem),
                (lam_h, lam), (bus_h, bus),
            ]
        )
    ]
    for cp in loads:
        cp.start()

    barrier = pltpu.get_barrier_semaphore()

    def greet(dev):
        pl.semaphore_signal(barrier, inc=1, device_id=dev, device_id_type=MESH)

    greet(nxt)
    greet(prv)
    greet((twin, 0))
    greet((twin, 1))

    @pl.loop(1, n_a)
    def _(d):
        greet(peer_a(d))

    @pl.loop(1, nz)
    def _(d):
        greet(peer_b(d))

    nlb = lines // 128
    flat = table.reshape(buses * nlb, 128)
    eye = (
        lax.broadcasted_iota(jnp.int32, (256, 256), 0)
        == lax.broadcasted_iota(jnp.int32, (256, 256), 1)
    ).astype(BF16)
    for c in range(nblk):
        if c % per_load == 0:
            ptdf_copies[c // per_load].wait()
        turned = lax.dot_general(
            eye, ptdf[:, c * 256 : (c + 1) * 256], (((1,), (1,)), ((), ())),
            preferred_element_type=F32,
        )
        for j in range(nlb):
            flat[pl.ds(c * 256 * nlb + j, 256, stride=nlb), :] = turned[:, j * 128 : (j + 1) * 128]

    for cp in loads:
        cp.wait()
    yb[0, gen] = yv[...].astype(BF16)
    pl.semaphore_wait(barrier, n_a - 1 + nz - 1 + 4)

    def send(src, dst, ssem, rsem, dev):
        return pltpu.make_async_remote_copy(
            src, dst, ssem, rsem, device_id=dev, device_id_type=MESH
        )

    def send_row(k, src, dst, dev):
        return pltpu.make_async_remote_copy(
            src, dst, row_send.at[k], row_recv.at[k], device_id=dev, device_id_type=MESH
        )

    yb_copy = send(yb.at[0, gen], yb.at[0, gen], yb_send, yb_recv, partner)
    yb_copy.start()
    mu_copy = send_row(0, muv.at[pl.ds(0, 1)], mu_next, prv)
    mu_copy.start()
    moves = [
        send(src.at[part], dst.at[part], init_send.at[i], init_recv.at[i], (twin, dev))
        for i, (src, dst, part, dev) in enumerate(
            [(y_h, yt, top, gen), (y_h, yt, low, other), (base_h, bt, top, gen), (base_h, bt, low, other)]
        )
    ]
    moves.append(send(lim_h, lim_x, init_send.at[4], init_recv.at[4], (twin, other)))
    for cp in moves:
        cp.start()

    group = 16
    n_group = 128 // group

    @pl.loop(0, gl // 128)
    def _(i):
        def fetch(s, k):
            stage[pl.ds((s * group + k) * nlb, nlb), :] = table[bus[i, s * group + k]]

        def pack(s, j):
            g0 = pl.multiple_of(i * 128 + s * group, group)
            got = stage[pl.ds(s * group * nlb + j, group, stride=nlb), :]
            fac[j // (nlb // 2), pl.ds(g0, group), pl.ds((j % (nlb // 2)) * 128, 128)] = got.astype(BF16)

        for k in range(group):
            fetch(0, k)
        for s in range(n_group):
            per = group // nlb
            for j in range(nlb):
                if s + 1 < n_group:
                    for k in range(per):
                        fetch(s + 1, j * per + k)
                pack(s, j)

    eye_r = lax.broadcasted_iota(jnp.int32, (rows, rows), 0) == lax.broadcasted_iota(
        jnp.int32, (rows, rows), 1
    )

    def to_column(row):
        return jnp.sum(jnp.where(eye_r, jnp.broadcast_to(row, (rows, rows)), 0.0), axis=1, keepdims=True)

    def to_row(col):
        return jnp.sum(jnp.where(eye_r, jnp.broadcast_to(col, (rows, rows)), 0.0), axis=0, keepdims=True)

    last = tm == ntm - 1
    first = tm == 0
    lam_col = to_column(lam[...])
    dem_col = to_column(dem[...])
    yb_copy.wait()
    mu_copy.wait()
    muv[pl.ds(rows, 1), :] = jnp.where(last, 0.0, mu_next[...])

    gc = 512
    sums = []
    for it in range(ITERS):
        acc_p[...] = jnp.zeros_like(acc_p)
        acc_d[...] = jnp.zeros_like(acc_d)
        acc_t[...] = jnp.zeros_like(acc_t)
        wlam = w * lam_col

        @pl.loop(0, gl // gc)
        def _(c):
            sl = pl.ds(pl.multiple_of(c * gc, gc), gc)
            pulled = lax.dot_general(
                yb[it, 0], fac[0, sl, :], (((1,), (1,)), ((), ())), preferred_element_type=F32
            ) + lax.dot_general(
                yb[it, 1], fac[1, sl, :], (((1,), (1,)), ((), ())), preferred_element_type=F32
            )
            xc = xv[:, sl]
            grad = cost[:, sl] + wlam + pulled + muv[pl.ds(0, rows), sl] - muv[pl.ds(1, rows), sl]
            xn = jnp.clip(xc - TAU * grad, lo[:, sl], hi[:, sl])
            xb = 2.0 * xn - xc
            d = xn - xc
            d2 = d * d
            xv[:, sl] = xn
            xbv[pl.ds(8, rows), sl] = xb
            xbb[:, sl] = xb.astype(BF16)
            acc_p[...] += sum(d2[:, k * 128 : (k + 1) * 128] for k in range(gc // 128))
            acc_t[...] += sum(xb[:, k * 128 : (k + 1) * 128] for k in range(gc // 128))

        rows_out = [send_row(1 + 2 * it, xbv.at[pl.ds(8 + rows - 1, 1)], xb_prev.at[it], nxt)]
        if it < ITERS - 1:
            rows_out.append(send_row(2 + 2 * it, xbv.at[pl.ds(8, 1)], xb_next, prv))
        for cp in rows_out:
            cp.start()
        tot_col = w * jnp.sum(acc_t[...], axis=1, keepdims=True)
        f_copies = []
        for p in range(2):
            flow[it, p] = jnp.dot(xbb[...], fac[p], preferred_element_type=F32)
            for r, part in enumerate((top, low)):
                cp = send(
                    flow.at[it, p, part], frecv.at[it, gen, part], f_send.at[it, p * 2 + r],
                    f_recv.at[it, gen * 2 + r], (twin, p if r == 0 else 1 - p),
                )
                cp.start()
                f_copies.append(cp)
        tot[it, :, pl.ds(0, rows)] = to_row(tot_col)
        t_copy = send(tot.at[it], tot_x.at[it], t_send.at[it], t_recv.at[it], partner)
        t_copy.start()

        for cp in rows_out:
            cp.wait()
        xbv[pl.ds(7, 1), :] = jnp.where(first, pinit[...], xb_prev[it])
        if it < ITERS - 1:
            m_n = muv[pl.ds(rows, 1), :]
            u_n = m_n + SIGMA * (xb_next[...] - xbv[pl.ds(8 + rows - 1, 1), :])
            mn_n = u_n - jnp.clip(u_n, -SIGMA * ramp[...], SIGMA * ramp[...])
            muv[pl.ds(rows, 1), :] = jnp.where(last, 0.0, mn_n)

        @pl.loop(0, gl // gc)
        def _(c):
            sl = pl.ds(pl.multiple_of(c * gc, gc), gc)
            m = muv[pl.ds(0, rows), sl]
            u = m + SIGMA * (xbv[pl.ds(8, rows), sl] - xbv[pl.ds(7, rows), sl])
            r = SIGMA * ramp[:, sl]
            mn = u - jnp.clip(u, -r, r)
            if it < ITERS - 1:
                muv[pl.ds(0, rows), sl] = mn
            else:
                muo[:, sl] = mn
            d = mn - m
            d2 = d * d
            acc_d[...] += sum(d2[:, k * 128 : (k + 1) * 128] for k in range(gc // 128))

        t_copy.wait()
        totals = tot_col + to_column(tot_x[it, :, pl.ds(0, rows)])
        lam_new = lam_col + SIGMA * (totals - dem_col)
        dl = lam_new - lam_col
        lam_col = lam_new

        for cp in f_copies:
            cp.wait_send()
        for s in range(2):
            for r, part in enumerate((top, low)):
                send(
                    flow.at[it, 0, part], frecv.at[it, s, part], f_send.at[it, r],
                    f_recv.at[it, s * 2 + r], (twin, s),
                ).wait_recv()
        if it == 0:
            for cp in moves:
                cp.wait()
        half_rows = rows // 2
        for r, part in enumerate((top, low)):
            old = yt[part, :]
            v = old + SIGMA * (frecv[it, 0, part, :] + frecv[it, 1, part, :])
            bv = bt[part, :]
            lv = (lim if r == 0 else lim_x)[...]
            yn = v - jnp.clip(v, SIGMA * (bv - lv), SIGMA * (bv + lv))
            yt[part, :] = yn
            if it < ITERS - 1:
                ybs[part, :] = yn.astype(BF16)
                for dev in range(2):
                    send(
                        ybs.at[part], yb.at[it + 1, gen if r == 0 else other, part],
                        ys_send.at[dev * 2 + r], ys_recv.at[gen * 2 + r], (twin, dev),
                    ).start()
            dy = yn - old
            dy2 = dy * dy
            acc_d[pl.ds(r * half_rows, half_rows), :] += sum(
                dy2[:, k * 128 : (k + 1) * 128] for k in range(half // 128)
            )
        primal = jnp.sum(acc_p[...], keepdims=True) / (TAU * cells)
        dual = (
            jnp.sum(acc_d[...], keepdims=True)
            + jnp.where(gen == 0, jnp.sum(dl * dl, keepdims=True), 0.0)
        ) / (SIGMA * cells)
        sums += [primal, dual]
        if it < ITERS - 1:
            for s in range(2):
                for r, part in enumerate((top, low)):
                    piece = s if r == 0 else 1 - s
                    send(
                        ybs.at[part], yb.at[it + 1, piece, part], ys_send.at[s * 2 + r],
                        ys_recv.at[s * 2 + r], (twin, s),
                    ).wait()

    lane = lax.broadcasted_iota(jnp.int32, (1, 128), 1)
    packed = jnp.zeros((1, 128), F32)
    for k, s in enumerate(sums):
        packed = jnp.where(lane == k, s, packed)

    def all_sum(value, buf, k, n, mine, peer, between=None):
        msg[k] = value
        buf[mine] = value

        @pl.loop(1, n)
        def _(d):
            pltpu.make_async_remote_copy(
                msg.at[k], buf.at[mine], ar_send.at[k], ar_recv.at[k],
                device_id=peer(d), device_id_type=MESH,
            ).start()

        if between is not None:
            between()
        several = buf.at[pl.ds(0, n - 1)]
        pltpu.make_async_copy(several, several, ar_send.at[k]).wait()
        pltpu.make_async_copy(several, several, ar_recv.at[k]).wait()
        return jnp.sum(buf[...], axis=0)

    y_back = [
        send(yt.at[part], yo.at[part], yr_send.at[r], yr_recv.at[r], (twin, dev))
        for r, (part, dev) in enumerate(((top, gen), (low, other)))
    ]

    def return_y():
        for cp in y_back:
            cp.start()

    total = all_sum(packed, ar_a, 0, n_a, mine_a, peer_a, return_y)
    total = all_sum(total, ar_b, 1, nz, zz, peer_b)
    place = 2 * lax.broadcasted_iota(jnp.int32, (ITERS, 2), 0) + lax.broadcasted_iota(
        jnp.int32, (ITERS, 2), 1
    )
    result = jnp.zeros((ITERS, 2), F32)
    for k in range(2 * ITERS):
        one = jnp.sum(jnp.where(lane == k, total, 0.0), axis=1, keepdims=True)
        result = jnp.where(place == k, one, result)
    mov_o[...] = result
    lam_o[...] = to_row(lam_col)
    for cp in y_back:
        cp.wait()


def write_out(x, y, mu, lam, mov, x_h, y_h, mu_h, lam_h, mov_h, sem):
    copies = [
        pltpu.make_async_copy(s, d, sem.at[i])
        for i, (s, d) in enumerate(((x, x_h), (mu, mu_h), (y, y_h), (lam, lam_h), (mov, mov_h)))
    ]
    for cp in copies:
        cp.start()
    for cp in copies:
        cp.wait()


def on_device(ntm, plane, hours, gl_total,
              dispatch, cost, p_low, p_high, ramp_limit, p_init, demand, bus_of, ptdf, line_base,
              line_limit, line_dual, ramp_dual, balance_dual):
    rows, gl = dispatch.shape
    lines, buses = ptdf.shape
    half = lines // 2
    n_a = 2 * plane
    nz = ntm // plane
    row = lambda a: a.reshape(1, -1)
    hbm = pl.BlockSpec(memory_space=pltpu.HBM)
    vmem = pl.BlockSpec(memory_space=pltpu.VMEM)
    V = pltpu.VMEM
    S = pltpu.SemaphoreType.DMA
    shapes = ((rows, gl), (rows, half), (rows, gl), (1, rows), (ITERS, 2))
    args = (
        bus_of.reshape(-1, 128), dispatch, row(cost), row(p_low), row(p_high), row(ramp_limit), row(p_init),
        row(demand), ptdf, line_base, row(line_limit), line_dual, ramp_dual, row(balance_dual),
    )
    state = pl.pallas_call(
        functools.partial(kernel, (ntm, plane, gl_total, hours)),
        name="dispatch_step",
        out_shape=tuple(V(shape, F32) for shape in shapes),
        in_specs=[hbm] * len(args),
        out_specs=(vmem,) * len(shapes),
        scratch_shapes=[
            V((lines, buses), BF16),
            V((buses, lines // 128, 128), F32),
            V((128 * (lines // 128), 128), F32),
            V((2, gl, half), BF16),
            V((rows + 8, gl), F32),
            V((rows + 8, gl), F32),
            V((rows, gl), BF16),
            V((rows, half), F32),
            V((rows, half), F32),
            V((rows, half), F32),
            V((ITERS, 2, rows, half), F32),
            V((ITERS, 2, rows, half), BF16),
            V((rows, half), BF16),
            V((ITERS, 2, rows, half), F32),
            pltpu.SMEM((gl // 128, 128), jnp.int32),
            V((1, gl), F32), V((1, gl), F32), V((1, gl), F32), V((1, gl), F32), V((1, gl), F32),
            V((1, half), F32), V((1, half), F32), V((1, rows), F32), V((1, rows), F32),
            V((1, gl), F32), V((ITERS, 1, gl), F32), V((1, gl), F32), V((ITERS, 1, 128), F32), V((ITERS, 1, 128), F32),
            V((rows, 128), F32), V((rows, 128), F32), V((rows, 128), F32),
            V((2, 1, 128), F32), V((n_a, 1, 128), F32), V((nz, 1, 128), F32),
            S((12,)), S((2,)), S, S, S((5,)), S((5,)), S((ITERS, 4)), S((ITERS, 4)), S((ITERS,)), S((ITERS,)),
            S((4,)), S((4,)), S((2,)), S((2,)), S((2 * ITERS,)), S((2 * ITERS,)), S((2,)), S((2,)),
        ],
        compiler_params=pltpu.CompilerParams(
            collective_id=0, has_side_effects=True, vmem_limit_bytes=48 * 1024 * 1024
        ),
    )(*(pltpu.with_memory_space_constraint(a, pltpu.HBM) for a in args))
    x, y, mu, lam, mov = pl.pallas_call(
        write_out,
        name="write_out",
        out_shape=tuple(jax.ShapeDtypeStruct(shape, F32) for shape in shapes),
        in_specs=[vmem] * len(shapes),
        out_specs=(hbm,) * len(shapes),
        scratch_shapes=[S((len(shapes),))],
        compiler_params=pltpu.CompilerParams(vmem_limit_bytes=1024 * 1024),
    )(*(pltpu.with_memory_space_constraint(a, pltpu.VMEM) for a in state))
    return x, y, mu, lam.reshape(-1), mov


def solution(mesh):
    ntm = mesh.shape["tm"]
    plane = min(PLANE, ntm)

    def body(*args):
        return on_device(ntm, plane, args[0].shape[0] * ntm, args[0].shape[1] * mesh.shape["gen"], *args)

    in_specs = (
        P("tm", "gen"), P("gen"), P("gen"), P("gen"), P("gen"), P("gen"), P("tm"), P("gen"), P(),
        P("tm", "gen"), P("gen"), P("tm", "gen"), P("tm", "gen"), P("tm"),
    )
    out_specs = (P("tm", "gen"), P("tm", "gen"), P("tm", "gen"), P("tm"), P())
    return jax.shard_map(body, mesh=mesh, in_specs=in_specs, out_specs=out_specs, check_vma=False)
```

```python
import functools
import math

import jax
import jax.numpy as jnp
from jax import lax
from jax.experimental import pallas as pl
from jax.experimental.pallas import tpu as pltpu
from jax.sharding import PartitionSpec as P

TAU = 0.35
SIGMA = 0.35
ITERS = 2
PLANE = 16
MESH = pl.DeviceIdType.MESH
BF16 = jnp.bfloat16
F32 = jnp.float32


def kernel(
    cfg,
    bus_h, x_h, cost_h, lo_h, hi_h, ramp_h, pinit_h, dem_h, ptdf_h, base_h, lim_h, y_h, mu_h, lam_h,
    xv, yo, muo, lam_o, mov_o,
    ptdf, table, stage, fac, muv, xbv, xbb, yv, yt, bt, flow, yb, ybs, frecv,
    bus, cost, lo, hi, ramp, pinit, lim, lim_x, dem, lam, mu_next, xb_prev, xb_next, tot, tot_x,
    acc_p, acc_d, acc_t, msg, ar_a, ar_b,
    load_sem, ptdf_sem, yb_send, yb_recv, init_send, init_recv, f_send, f_recv, t_send, t_recv,
    ys_send, ys_recv, yr_send, yr_recv, row_send, row_recv, ar_send, ar_recv,
):
    ntm, plane, gl_total, hours = cfg
    rows, gl = x_h.shape
    lines, buses = ptdf_h.shape
    half = lines // 2
    nz = ntm // plane
    w = 1.0 / math.sqrt(gl_total)
    cells = float(hours) * float(gl_total)
    tm = lax.axis_index("tm")
    gen = lax.axis_index("gen")
    other = 1 - gen
    partner = (tm, other)
    nxt = (lax.rem(tm + 1, ntm), gen)
    prv = (lax.rem(tm + ntm - 1, ntm), gen)
    twin = tm + 2 - 4 * lax.rem(tm // 2, 2)
    top = pl.ds(0, rows // 2)
    low = pl.ds(rows // 2, rows // 2)
    zz = tm // plane
    in_plane = lax.rem(tm, plane)
    n_a = 2 * plane
    mine_a = in_plane * 2 + gen

    def peer_a(d):
        q = lax.rem(mine_a + d, n_a)
        return (zz * plane + q // 2, lax.rem(q, 2))

    def peer_b(d):
        return (lax.rem(zz + d, nz) * plane + in_plane, gen)

    nblk = buses // 256
    per_load = nblk // 2
    ptdf_copies = []
    for c in range(2):
        part = pl.ds(c * per_load * 256, per_load * 256)
        cp = pltpu.make_async_copy(ptdf_h.at[:, part], ptdf.at[:, part], ptdf_sem.at[c])
        cp.start()
        ptdf_copies.append(cp)
    loads = [
        pltpu.make_async_copy(s, d, load_sem.at[i])
        for i, (s, d) in enumerate(
            [
                (y_h, yv), (mu_h, muv.at[pl.ds(0, rows)]), (x_h, xv), (cost_h, cost),
                (lo_h, lo), (hi_h, hi), (ramp_h, ramp), (pinit_h, pinit), (lim_h, lim), (dem_h, dem),
                (lam_h, lam), (bus_h, bus),
            ]
        )
    ]
    for cp in loads:
        cp.start()

    barrier = pltpu.get_barrier_semaphore()

    def greet(dev):
        pl.semaphore_signal(barrier, inc=1, device_id=dev, device_id_type=MESH)

    greet(nxt)
    greet(prv)
    greet((twin, 0))
    greet((twin, 1))

    @pl.loop(1, n_a)
    def _(d):
        greet(peer_a(d))

    @pl.loop(1, nz)
    def _(d):
        greet(peer_b(d))

    nlb = lines // 128
    flat = table.reshape(buses * nlb, 128)
    eye = (
        lax.broadcasted_iota(jnp.int32, (256, 256), 0)
        == lax.broadcasted_iota(jnp.int32, (256, 256), 1)
    ).astype(BF16)
    for c in range(nblk):
        if c % per_load == 0:
            ptdf_copies[c // per_load].wait()
        turned = lax.dot_general(
            eye, ptdf[:, c * 256 : (c + 1) * 256], (((1,), (1,)), ((), ())),
            preferred_element_type=F32,
        )
        for j in range(nlb):
            flat[pl.ds(c * 256 * nlb + j, 256, stride=nlb), :] = turned[:, j * 128 : (j + 1) * 128]

    for cp in loads:
        cp.wait()
    yb[0, gen] = yv[...].astype(BF16)
    pl.semaphore_wait(barrier, n_a - 1 + nz - 1 + 4)

    def send(src, dst, ssem, rsem, dev):
        return pltpu.make_async_remote_copy(
            src, dst, ssem, rsem, device_id=dev, device_id_type=MESH
        )

    def send_row(k, src, dst, dev):
        return pltpu.make_async_remote_copy(
            src, dst, row_send.at[k], row_recv.at[k], device_id=dev, device_id_type=MESH
        )

    yb_copy = send(yb.at[0, gen], yb.at[0, gen], yb_send, yb_recv, partner)
    yb_copy.start()
    mu_copy = send_row(0, muv.at[pl.ds(0, 1)], mu_next, prv)
    mu_copy.start()
    moves = [
        send(src.at[part], dst.at[part], init_send.at[i], init_recv.at[i], (twin, dev))
        for i, (src, dst, part, dev) in enumerate(
            [(y_h, yt, top, gen), (y_h, yt, low, other), (base_h, bt, top, gen), (base_h, bt, low, other)]
        )
    ]
    moves.append(send(lim_h, lim_x, init_send.at[4], init_recv.at[4], (twin, other)))
    for cp in moves:
        cp.start()

    group = 16
    n_group = 128 // group

    @pl.loop(0, gl // 128)
    def _(i):
        def fetch(s, k):
            stage[pl.ds((s * group + k) * nlb, nlb), :] = table[bus[i, s * group + k]]

        def pack(s, j):
            g0 = pl.multiple_of(i * 128 + s * group, group)
            got = stage[pl.ds(s * group * nlb + j, group, stride=nlb), :]
            fac[j // (nlb // 2), pl.ds(g0, group), pl.ds((j % (nlb // 2)) * 128, 128)] = got.astype(BF16)

        for k in range(group):
            fetch(0, k)
        for s in range(n_group):
            per = group // nlb
            for j in range(nlb):
                if s + 1 < n_group:
                    for k in range(per):
                        fetch(s + 1, j * per + k)
                pack(s, j)

    eye_r = lax.broadcasted_iota(jnp.int32, (rows, rows), 0) == lax.broadcasted_iota(
        jnp.int32, (rows, rows), 1
    )

    def to_column(row):
        return jnp.sum(jnp.where(eye_r, jnp.broadcast_to(row, (rows, rows)), 0.0), axis=1, keepdims=True)

    def to_row(col):
        return jnp.sum(jnp.where(eye_r, jnp.broadcast_to(col, (rows, rows)), 0.0), axis=0, keepdims=True)

    last = tm == ntm - 1
    first = tm == 0
    lam_col = to_column(lam[...])
    dem_col = to_column(dem[...])
    yb_copy.wait()
    mu_copy.wait()
    muv[pl.ds(rows, 1), :] = jnp.where(last, 0.0, mu_next[...])

    gc = 512
    sums = []
    for it in range(ITERS):
        acc_p[...] = jnp.zeros_like(acc_p)
        acc_d[...] = jnp.zeros_like(acc_d)
        acc_t[...] = jnp.zeros_like(acc_t)
        wlam = w * lam_col

        y_t = jnp.concatenate([yb[it, h].astype(F32).T.astype(BF16) for h in range(2)], axis=0)
        for c in range(gl // gc):
            sl = pl.ds(c * gc, gc)
            pulled_t = jnp.dot(fac[0, sl, :], y_t[:half], preferred_element_type=F32) + jnp.dot(
                fac[1, sl, :], y_t[half:], preferred_element_type=F32
            )
            pulled = pulled_t.T
            xc = xv[:, sl]
            grad = cost[:, sl] + wlam + pulled + muv[pl.ds(0, rows), sl] - muv[pl.ds(1, rows), sl]
            xn = jnp.clip(xc - TAU * grad, lo[:, sl], hi[:, sl])
            xb = 2.0 * xn - xc
            d = xn - xc
            d2 = d * d
            xv[:, sl] = xn
            xbv[pl.ds(8, rows), sl] = xb
            xbb[:, sl] = xb.astype(BF16)
            acc_p[...] += sum(d2[:, k * 128 : (k + 1) * 128] for k in range(gc // 128))
            acc_t[...] += sum(xb[:, k * 128 : (k + 1) * 128] for k in range(gc // 128))

        rows_out = [send_row(1 + 2 * it, xbv.at[pl.ds(8 + rows - 1, 1)], xb_prev.at[it], nxt)]
        if it < ITERS - 1:
            rows_out.append(send_row(2 + 2 * it, xbv.at[pl.ds(8, 1)], xb_next, prv))
        for cp in rows_out:
            cp.start()
        tot_col = w * jnp.sum(acc_t[...], axis=1, keepdims=True)
        tot[it, :, pl.ds(0, rows)] = to_row(tot_col)
        t_copy = send(tot.at[it], tot_x.at[it], t_send.at[it], t_recv.at[it], partner)
        t_copy.start()
        f_copies = []
        for p in range(2):
            flow[it, p] = jnp.dot(xbb[...], fac[p], preferred_element_type=F32)
            for r, part in enumerate((top, low)):
                cp = send(
                    flow.at[it, p, part], frecv.at[it, gen, part], f_send.at[it, p * 2 + r],
                    f_recv.at[it, gen * 2 + r], (twin, p if r == 0 else 1 - p),
                )
                cp.start()
                f_copies.append(cp)
        for cp in rows_out:
            cp.wait()
        xbv[pl.ds(7, 1), :] = jnp.where(first, pinit[...], xb_prev[it])
        if it < ITERS - 1:
            m_n = muv[pl.ds(rows, 1), :]
            u_n = m_n + SIGMA * (xb_next[...] - xbv[pl.ds(8 + rows - 1, 1), :])
            mn_n = u_n - jnp.clip(u_n, -SIGMA * ramp[...], SIGMA * ramp[...])
            muv[pl.ds(rows, 1), :] = jnp.where(last, 0.0, mn_n)

        @pl.loop(0, gl // gc)
        def _(c):
            sl = pl.ds(pl.multiple_of(c * gc, gc), gc)
            m = muv[pl.ds(0, rows), sl]
            u = m + SIGMA * (xbv[pl.ds(8, rows), sl] - xbv[pl.ds(7, rows), sl])
            r = SIGMA * ramp[:, sl]
            mn = u - jnp.clip(u, -r, r)
            if it < ITERS - 1:
                muv[pl.ds(0, rows), sl] = mn
            else:
                muo[:, sl] = mn
            d = mn - m
            d2 = d * d
            acc_d[...] += sum(d2[:, k * 128 : (k + 1) * 128] for k in range(gc // 128))

        t_copy.wait()
        totals = tot_col + to_column(tot_x[it, :, pl.ds(0, rows)])
        lam_new = lam_col + SIGMA * (totals - dem_col)
        dl = lam_new - lam_col
        lam_col = lam_new

        for cp in f_copies:
            cp.wait_send()
        for s in range(2):
            for r, part in enumerate((top, low)):
                send(
                    flow.at[it, 0, part], frecv.at[it, s, part], f_send.at[it, r],
                    f_recv.at[it, s * 2 + r], (twin, s),
                ).wait_recv()
        if it == 0:
            for cp in moves:
                cp.wait()
        half_rows = rows // 2
        for r, part in enumerate((top, low)):
            old = yt[part, :]
            v = old + SIGMA * (frecv[it, 0, part, :] + frecv[it, 1, part, :])
            bv = bt[part, :]
            lv = (lim if r == 0 else lim_x)[...]
            yn = v - jnp.clip(v, SIGMA * (bv - lv), SIGMA * (bv + lv))
            yt[part, :] = yn
            if it < ITERS - 1:
                ybs[part, :] = yn.astype(BF16)
                for dev in range(2):
                    send(
                        ybs.at[part], yb.at[it + 1, gen if r == 0 else other, part],
                        ys_send.at[dev * 2 + r], ys_recv.at[gen * 2 + r], (twin, dev),
                    ).start()
            dy = yn - old
            dy2 = dy * dy
            acc_d[pl.ds(r * half_rows, half_rows), :] += sum(
                dy2[:, k * 128 : (k + 1) * 128] for k in range(half // 128)
            )
        primal = jnp.sum(acc_p[...], keepdims=True) / (TAU * cells)
        dual = (
            jnp.sum(acc_d[...], keepdims=True)
            + jnp.where(gen == 0, jnp.sum(dl * dl, keepdims=True), 0.0)
        ) / (SIGMA * cells)
        sums += [primal, dual]
        if it < ITERS - 1:
            for s in range(2):
                for r, part in enumerate((top, low)):
                    piece = s if r == 0 else 1 - s
                    send(
                        ybs.at[part], yb.at[it + 1, piece, part], ys_send.at[s * 2 + r],
                        ys_recv.at[s * 2 + r], (twin, s),
                    ).wait()

    lane = lax.broadcasted_iota(jnp.int32, (1, 128), 1)
    packed = jnp.zeros((1, 128), F32)
    for k, s in enumerate(sums):
        packed = jnp.where(lane == k, s, packed)

    def all_sum(value, buf, k, n, mine, peer, between=None):
        msg[k] = value
        buf[mine] = value

        @pl.loop(1, n)
        def _(d):
            pltpu.make_async_remote_copy(
                msg.at[k], buf.at[mine], ar_send.at[k], ar_recv.at[k],
                device_id=peer(d), device_id_type=MESH,
            ).start()

        if between is not None:
            between()
        several = buf.at[pl.ds(0, n - 1)]
        pltpu.make_async_copy(several, several, ar_send.at[k]).wait()
        pltpu.make_async_copy(several, several, ar_recv.at[k]).wait()
        return jnp.sum(buf[...], axis=0)

    y_back = [
        send(yt.at[part], yo.at[part], yr_send.at[r], yr_recv.at[r], (twin, dev))
        for r, (part, dev) in enumerate(((top, gen), (low, other)))
    ]

    def return_y():
        for cp in y_back:
            cp.start()

    total = all_sum(packed, ar_a, 0, n_a, mine_a, peer_a, return_y)
    total = all_sum(total, ar_b, 1, nz, zz, peer_b)
    place = 2 * lax.broadcasted_iota(jnp.int32, (ITERS, 2), 0) + lax.broadcasted_iota(
        jnp.int32, (ITERS, 2), 1
    )
    result = jnp.zeros((ITERS, 2), F32)
    for k in range(2 * ITERS):
        one = jnp.sum(jnp.where(lane == k, total, 0.0), axis=1, keepdims=True)
        result = jnp.where(place == k, one, result)
    mov_o[...] = result
    lam_o[...] = to_row(lam_col)
    for cp in y_back:
        cp.wait()


def write_out(x, y, mu, lam, mov, x_h, y_h, mu_h, lam_h, mov_h, sem):
    copies = [
        pltpu.make_async_copy(s, d, sem.at[i])
        for i, (s, d) in enumerate(((x, x_h), (mu, mu_h), (y, y_h), (lam, lam_h), (mov, mov_h)))
    ]
    for cp in copies:
        cp.start()
    for cp in copies:
        cp.wait()


def on_device(ntm, plane, hours, gl_total,
              dispatch, cost, p_low, p_high, ramp_limit, p_init, demand, bus_of, ptdf, line_base,
              line_limit, line_dual, ramp_dual, balance_dual):
    rows, gl = dispatch.shape
    lines, buses = ptdf.shape
    half = lines // 2
    n_a = 2 * plane
    nz = ntm // plane
    row = lambda a: a.reshape(1, -1)
    hbm = pl.BlockSpec(memory_space=pltpu.HBM)
    vmem = pl.BlockSpec(memory_space=pltpu.VMEM)
    V = pltpu.VMEM
    S = pltpu.SemaphoreType.DMA
    shapes = ((rows, gl), (rows, half), (rows, gl), (1, rows), (ITERS, 2))
    args = (
        bus_of.reshape(-1, 128), dispatch, row(cost), row(p_low), row(p_high), row(ramp_limit), row(p_init),
        row(demand), ptdf, line_base, row(line_limit), line_dual, ramp_dual, row(balance_dual),
    )
    state = pl.pallas_call(
        functools.partial(kernel, (ntm, plane, gl_total, hours)),
        name="dispatch_step",
        out_shape=tuple(V(shape, F32) for shape in shapes),
        in_specs=[hbm] * len(args),
        out_specs=(vmem,) * len(shapes),
        scratch_shapes=[
            V((lines, buses), BF16),
            V((buses, lines // 128, 128), F32),
            V((128 * (lines // 128), 128), F32),
            V((2, gl, half), BF16),
            V((rows + 8, gl), F32),
            V((rows + 8, gl), F32),
            V((rows, gl), BF16),
            V((rows, half), F32),
            V((rows, half), F32),
            V((rows, half), F32),
            V((ITERS, 2, rows, half), F32),
            V((ITERS, 2, rows, half), BF16),
            V((rows, half), BF16),
            V((ITERS, 2, rows, half), F32),
            pltpu.SMEM((gl // 128, 128), jnp.int32),
            V((1, gl), F32), V((1, gl), F32), V((1, gl), F32), V((1, gl), F32), V((1, gl), F32),
            V((1, half), F32), V((1, half), F32), V((1, rows), F32), V((1, rows), F32),
            V((1, gl), F32), V((ITERS, 1, gl), F32), V((1, gl), F32), V((ITERS, 1, 128), F32), V((ITERS, 1, 128), F32),
            V((rows, 128), F32), V((rows, 128), F32), V((rows, 128), F32),
            V((2, 1, 128), F32), V((n_a, 1, 128), F32), V((nz, 1, 128), F32),
            S((12,)), S((2,)), S, S, S((5,)), S((5,)), S((ITERS, 4)), S((ITERS, 4)), S((ITERS,)), S((ITERS,)),
            S((4,)), S((4,)), S((2,)), S((2,)), S((2 * ITERS,)), S((2 * ITERS,)), S((2,)), S((2,)),
        ],
        compiler_params=pltpu.CompilerParams(
            collective_id=0, has_side_effects=True, vmem_limit_bytes=48 * 1024 * 1024
        ),
    )(*(pltpu.with_memory_space_constraint(a, pltpu.HBM) for a in args))
    x, y, mu, lam, mov = pl.pallas_call(
        write_out,
        name="write_out",
        out_shape=tuple(jax.ShapeDtypeStruct(shape, F32) for shape in shapes),
        in_specs=[vmem] * len(shapes),
        out_specs=(hbm,) * len(shapes),
        scratch_shapes=[S((len(shapes),))],
        compiler_params=pltpu.CompilerParams(vmem_limit_bytes=1024 * 1024),
    )(*(pltpu.with_memory_space_constraint(a, pltpu.VMEM) for a in state))
    return x, y, mu, lam.reshape(-1), mov


def solution(mesh):
    ntm = mesh.shape["tm"]
    plane = min(PLANE, ntm)

    def body(*args):
        return on_device(ntm, plane, args[0].shape[0] * ntm, args[0].shape[1] * mesh.shape["gen"], *args)

    in_specs = (
        P("tm", "gen"), P("gen"), P("gen"), P("gen"), P("gen"), P("gen"), P("tm"), P("gen"), P(),
        P("tm", "gen"), P("gen"), P("tm", "gen"), P("tm", "gen"), P("tm"),
    )
    out_specs = (P("tm", "gen"), P("tm", "gen"), P("tm", "gen"), P("tm"), P())
    return jax.shard_map(body, mesh=mesh, in_specs=in_specs, out_specs=out_specs, check_vma=False)
```

```python
import functools
import math

import jax
import jax.numpy as jnp
from jax import lax
from jax.experimental import pallas as pl
from jax.experimental.pallas import tpu as pltpu
from jax.sharding import PartitionSpec as P

TAU = 0.35
SIGMA = 0.35
ITERS = 2
PLANE = 16
MESH = pl.DeviceIdType.MESH
BF16 = jnp.bfloat16
F32 = jnp.float32
STEPS = 32767.0


def kernel(
    cfg,
    bus_h, x_h, cost_h, lo_h, hi_h, ramp_h, pinit_h, dem_h, ptdf_h, base_h, lim_h, y_h, mu_h, lam_h,
    xv, yo, muo, lam_o, mov_o,
    ptdf, table, stage, fac, muv, xbv, xbb, yv, yt, bt, flow, yb, ybs, frecv, scale, scale_x,
    bus, cost, lo, hi, ramp, pinit, lim, lim_x, dem, lam, mu_next, xb_prev, xb_next, tot, tot_x,
    acc_p, acc_d, acc_t, msg, ar_a, ar_b,
    load_sem, ptdf_sem, yb_send, yb_recv, init_send, init_recv, f_send, f_recv, s_send, s_recv, t_send, t_recv,
    ys_send, ys_recv, yr_send, yr_recv, row_send, row_recv, ar_send, ar_recv,
):
    ntm, plane, gl_total, hours = cfg
    rows, gl = x_h.shape
    lines, buses = ptdf_h.shape
    half = lines // 2
    nz = ntm // plane
    w = 1.0 / math.sqrt(gl_total)
    cells = float(hours) * float(gl_total)
    tm = lax.axis_index("tm")
    gen = lax.axis_index("gen")
    other = 1 - gen
    partner = (tm, other)
    nxt = (lax.rem(tm + 1, ntm), gen)
    prv = (lax.rem(tm + ntm - 1, ntm), gen)
    twin = tm + 2 - 4 * lax.rem(tm // 2, 2)
    top = pl.ds(0, rows // 2)
    low = pl.ds(rows // 2, rows // 2)
    zz = tm // plane
    in_plane = lax.rem(tm, plane)
    n_a = 2 * plane
    mine_a = in_plane * 2 + gen

    def peer_a(d):
        q = lax.rem(mine_a + d, n_a)
        return (zz * plane + q // 2, lax.rem(q, 2))

    def peer_b(d):
        return (lax.rem(zz + d, nz) * plane + in_plane, gen)

    nblk = buses // 256
    per_load = nblk // 2
    ptdf_copies = []
    for c in range(2):
        part = pl.ds(c * per_load * 256, per_load * 256)
        cp = pltpu.make_async_copy(ptdf_h.at[:, part], ptdf.at[:, part], ptdf_sem.at[c])
        cp.start()
        ptdf_copies.append(cp)
    loads = [
        pltpu.make_async_copy(s, d, load_sem.at[i])
        for i, (s, d) in enumerate(
            [
                (y_h, yv), (mu_h, muv.at[pl.ds(0, rows)]), (x_h, xv), (cost_h, cost),
                (lo_h, lo), (hi_h, hi), (ramp_h, ramp), (pinit_h, pinit), (lim_h, lim), (dem_h, dem),
                (lam_h, lam), (bus_h, bus),
            ]
        )
    ]
    for cp in loads:
        cp.start()

    barrier = pltpu.get_barrier_semaphore()

    def greet(dev):
        pl.semaphore_signal(barrier, inc=1, device_id=dev, device_id_type=MESH)

    greet(nxt)
    greet(prv)
    greet((twin, 0))
    greet((twin, 1))

    @pl.loop(1, n_a)
    def _(d):
        greet(peer_a(d))

    @pl.loop(1, nz)
    def _(d):
        greet(peer_b(d))

    nlb = lines // 128
    flat = table.reshape(buses * nlb, 128)
    eye = (
        lax.broadcasted_iota(jnp.int32, (256, 256), 0)
        == lax.broadcasted_iota(jnp.int32, (256, 256), 1)
    ).astype(BF16)
    for c in range(nblk):
        if c % per_load == 0:
            ptdf_copies[c // per_load].wait()
        turned = lax.dot_general(
            eye, ptdf[:, c * 256 : (c + 1) * 256], (((1,), (1,)), ((), ())),
            preferred_element_type=F32,
        )
        for j in range(nlb):
            flat[pl.ds(c * 256 * nlb + j, 256, stride=nlb), :] = turned[:, j * 128 : (j + 1) * 128]

    for cp in loads:
        cp.wait()
    yb[0, gen] = yv[...].astype(BF16)
    pl.semaphore_wait(barrier, n_a - 1 + nz - 1 + 4)

    def send(src, dst, ssem, rsem, dev):
        return pltpu.make_async_remote_copy(
            src, dst, ssem, rsem, device_id=dev, device_id_type=MESH
        )

    def send_row(k, src, dst, dev):
        return pltpu.make_async_remote_copy(
            src, dst, row_send.at[k], row_recv.at[k], device_id=dev, device_id_type=MESH
        )

    yb_copy = send(yb.at[0, gen], yb.at[0, gen], yb_send, yb_recv, partner)
    yb_copy.start()
    mu_copy = send_row(0, muv.at[pl.ds(0, 1)], mu_next, prv)
    mu_copy.start()
    moves = [
        send(src.at[part], dst.at[part], init_send.at[i], init_recv.at[i], (twin, dev))
        for i, (src, dst, part, dev) in enumerate(
            [(y_h, yt, top, gen), (y_h, yt, low, other), (base_h, bt, top, gen), (base_h, bt, low, other)]
        )
    ]
    moves.append(send(lim_h, lim_x, init_send.at[4], init_recv.at[4], (twin, other)))
    for cp in moves:
        cp.start()

    group = 16
    n_group = 128 // group

    @pl.loop(0, gl // 128)
    def _(i):
        def fetch(s, k):
            stage[pl.ds((s * group + k) * nlb, nlb), :] = table[bus[i, s * group + k]]

        def pack(s, j):
            g0 = pl.multiple_of(i * 128 + s * group, group)
            got = stage[pl.ds(s * group * nlb + j, group, stride=nlb), :]
            fac[j // (nlb // 2), pl.ds(g0, group), pl.ds((j % (nlb // 2)) * 128, 128)] = got.astype(BF16)

        for k in range(group):
            fetch(0, k)
        for s in range(n_group):
            per = group // nlb
            for j in range(nlb):
                if s + 1 < n_group:
                    for k in range(per):
                        fetch(s + 1, j * per + k)
                pack(s, j)

    eye_r = lax.broadcasted_iota(jnp.int32, (rows, rows), 0) == lax.broadcasted_iota(
        jnp.int32, (rows, rows), 1
    )

    def to_column(row):
        return jnp.sum(jnp.where(eye_r, jnp.broadcast_to(row, (rows, rows)), 0.0), axis=1, keepdims=True)

    def to_row(col):
        return jnp.sum(jnp.where(eye_r, jnp.broadcast_to(col, (rows, rows)), 0.0), axis=0, keepdims=True)

    last = tm == ntm - 1
    first = tm == 0
    lam_col = to_column(lam[...])
    dem_col = to_column(dem[...])
    yb_copy.wait()
    mu_copy.wait()
    muv[pl.ds(rows, 1), :] = jnp.where(last, 0.0, mu_next[...])

    gc = 512
    sums = []
    for it in range(ITERS):
        acc_p[...] = jnp.zeros_like(acc_p)
        acc_d[...] = jnp.zeros_like(acc_d)
        acc_t[...] = jnp.zeros_like(acc_t)
        wlam = w * lam_col

        y_t = jnp.concatenate([yb[it, h].astype(F32).T.astype(BF16) for h in range(2)], axis=0)
        for c in range(gl // gc):
            sl = pl.ds(c * gc, gc)
            pulled_t = jnp.dot(fac[0, sl, :], y_t[:half], preferred_element_type=F32) + jnp.dot(
                fac[1, sl, :], y_t[half:], preferred_element_type=F32
            )
            pulled = pulled_t.T
            xc = xv[:, sl]
            grad = cost[:, sl] + wlam + pulled + muv[pl.ds(0, rows), sl] - muv[pl.ds(1, rows), sl]
            xn = jnp.clip(xc - TAU * grad, lo[:, sl], hi[:, sl])
            xb = 2.0 * xn - xc
            d = xn - xc
            d2 = d * d
            xv[:, sl] = xn
            xbv[pl.ds(8, rows), sl] = xb
            xbb[:, sl] = xb.astype(BF16)
            acc_p[...] += sum(d2[:, k * 128 : (k + 1) * 128] for k in range(gc // 128))
            acc_t[...] += sum(xb[:, k * 128 : (k + 1) * 128] for k in range(gc // 128))

        rows_out = [send_row(1 + 2 * it, xbv.at[pl.ds(8 + rows - 1, 1)], xb_prev.at[it], nxt)]
        if it < ITERS - 1:
            rows_out.append(send_row(2 + 2 * it, xbv.at[pl.ds(8, 1)], xb_next, prv))
        for cp in rows_out:
            cp.start()
        tot_col = w * jnp.sum(acc_t[...], axis=1, keepdims=True)
        tot[it, :, pl.ds(0, rows)] = to_row(tot_col)
        t_copy = send(tot.at[it], tot_x.at[it], t_send.at[it], t_recv.at[it], partner)
        t_copy.start()
        f_copies = []
        for p in range(2):
            sums_p = jnp.dot(xbb[...], fac[p], preferred_element_type=F32)
            for r, part in enumerate((top, low)):
                block = sums_p[r * (rows // 2) : (r + 1) * (rows // 2)]
                largest = jnp.maximum(jnp.max(jnp.abs(block), axis=0, keepdims=True), 1e-30)
                flow[it, p, part] = jnp.round(block * (STEPS / largest)).astype(jnp.int32).astype(jnp.int16)
                scale[it, p, r] = largest * (1.0 / STEPS)
                dev = (twin, p if r == 0 else 1 - p)
                for cp in (
                    send(
                        scale.at[it, p, r], scale_x.at[it, gen, r], s_send.at[it, p * 2 + r],
                        s_recv.at[it, gen * 2 + r], dev,
                    ),
                    send(
                        flow.at[it, p, part], frecv.at[it, gen, part], f_send.at[it, p * 2 + r],
                        f_recv.at[it, gen * 2 + r], dev,
                    ),
                ):
                    cp.start()
                    f_copies.append(cp)
        for cp in rows_out:
            cp.wait()
        xbv[pl.ds(7, 1), :] = jnp.where(first, pinit[...], xb_prev[it])
        if it < ITERS - 1:
            m_n = muv[pl.ds(rows, 1), :]
            u_n = m_n + SIGMA * (xb_next[...] - xbv[pl.ds(8 + rows - 1, 1), :])
            mn_n = u_n - jnp.clip(u_n, -SIGMA * ramp[...], SIGMA * ramp[...])
            muv[pl.ds(rows, 1), :] = jnp.where(last, 0.0, mn_n)

        @pl.loop(0, gl // gc)
        def _(c):
            sl = pl.ds(pl.multiple_of(c * gc, gc), gc)
            m = muv[pl.ds(0, rows), sl]
            u = m + SIGMA * (xbv[pl.ds(8, rows), sl] - xbv[pl.ds(7, rows), sl])
            r = SIGMA * ramp[:, sl]
            mn = u - jnp.clip(u, -r, r)
            if it < ITERS - 1:
                muv[pl.ds(0, rows), sl] = mn
            else:
                muo[:, sl] = mn
            d = mn - m
            d2 = d * d
            acc_d[...] += sum(d2[:, k * 128 : (k + 1) * 128] for k in range(gc // 128))

        t_copy.wait()
        totals = tot_col + to_column(tot_x[it, :, pl.ds(0, rows)])
        lam_new = lam_col + SIGMA * (totals - dem_col)
        dl = lam_new - lam_col
        lam_col = lam_new

        for cp in f_copies:
            cp.wait_send()
        for s in range(2):
            for r, part in enumerate((top, low)):
                send(
                    scale.at[it, 0, r], scale_x.at[it, s, r], s_send.at[it, r],
                    s_recv.at[it, s * 2 + r], (twin, s),
                ).wait_recv()
                send(
                    flow.at[it, 0, part], frecv.at[it, s, part], f_send.at[it, r],
                    f_recv.at[it, s * 2 + r], (twin, s),
                ).wait_recv()
        if it == 0:
            for cp in moves:
                cp.wait()
        half_rows = rows // 2
        for r, part in enumerate((top, low)):
            old = yt[part, :]
            v = old + SIGMA * sum(
                frecv[it, s, part, :].astype(jnp.int32).astype(F32) * scale_x[it, s, r] for s in range(2)
            )
            bv = bt[part, :]
            lv = (lim if r == 0 else lim_x)[...]
            yn = v - jnp.clip(v, SIGMA * (bv - lv), SIGMA * (bv + lv))
            yt[part, :] = yn
            if it < ITERS - 1:
                ybs[part, :] = yn.astype(BF16)
                for dev in range(2):
                    send(
                        ybs.at[part], yb.at[it + 1, gen if r == 0 else other, part],
                        ys_send.at[dev * 2 + r], ys_recv.at[gen * 2 + r], (twin, dev),
                    ).start()
            dy = yn - old
            dy2 = dy * dy
            acc_d[pl.ds(r * half_rows, half_rows), :] += sum(
                dy2[:, k * 128 : (k + 1) * 128] for k in range(half // 128)
            )
        primal = jnp.sum(acc_p[...], keepdims=True) / (TAU * cells)
        dual = (
            jnp.sum(acc_d[...], keepdims=True)
            + jnp.where(gen == 0, jnp.sum(dl * dl, keepdims=True), 0.0)
        ) / (SIGMA * cells)
        sums += [primal, dual]
        if it < ITERS - 1:
            for s in range(2):
                for r, part in enumerate((top, low)):
                    piece = s if r == 0 else 1 - s
                    send(
                        ybs.at[part], yb.at[it + 1, piece, part], ys_send.at[s * 2 + r],
                        ys_recv.at[s * 2 + r], (twin, s),
                    ).wait()

    lane = lax.broadcasted_iota(jnp.int32, (1, 128), 1)
    packed = jnp.zeros((1, 128), F32)
    for k, s in enumerate(sums):
        packed = jnp.where(lane == k, s, packed)

    def all_sum(value, buf, k, n, mine, peer, between=None):
        msg[k] = value
        buf[mine] = value

        @pl.loop(1, n)
        def _(d):
            pltpu.make_async_remote_copy(
                msg.at[k], buf.at[mine], ar_send.at[k], ar_recv.at[k],
                device_id=peer(d), device_id_type=MESH,
            ).start()

        if between is not None:
            between()
        several = buf.at[pl.ds(0, n - 1)]
        pltpu.make_async_copy(several, several, ar_send.at[k]).wait()
        pltpu.make_async_copy(several, several, ar_recv.at[k]).wait()
        return jnp.sum(buf[...], axis=0)

    y_back = [
        send(yt.at[part], yo.at[part], yr_send.at[r], yr_recv.at[r], (twin, dev))
        for r, (part, dev) in enumerate(((top, gen), (low, other)))
    ]

    def return_y():
        for cp in y_back:
            cp.start()

    total = all_sum(packed, ar_a, 0, n_a, mine_a, peer_a, return_y)
    total = all_sum(total, ar_b, 1, nz, zz, peer_b)
    place = 2 * lax.broadcasted_iota(jnp.int32, (ITERS, 2), 0) + lax.broadcasted_iota(
        jnp.int32, (ITERS, 2), 1
    )
    result = jnp.zeros((ITERS, 2), F32)
    for k in range(2 * ITERS):
        one = jnp.sum(jnp.where(lane == k, total, 0.0), axis=1, keepdims=True)
        result = jnp.where(place == k, one, result)
    mov_o[...] = result
    lam_o[...] = to_row(lam_col)
    for cp in y_back:
        cp.wait()


def write_out(x, y, mu, lam, mov, x_h, y_h, mu_h, lam_h, mov_h, sem):
    copies = [
        pltpu.make_async_copy(s, d, sem.at[i])
        for i, (s, d) in enumerate(((x, x_h), (mu, mu_h), (y, y_h), (lam, lam_h), (mov, mov_h)))
    ]
    for cp in copies:
        cp.start()
    for cp in copies:
        cp.wait()


def on_device(ntm, plane, hours, gl_total,
              dispatch, cost, p_low, p_high, ramp_limit, p_init, demand, bus_of, ptdf, line_base,
              line_limit, line_dual, ramp_dual, balance_dual):
    rows, gl = dispatch.shape
    lines, buses = ptdf.shape
    half = lines // 2
    n_a = 2 * plane
    nz = ntm // plane
    row = lambda a: a.reshape(1, -1)
    hbm = pl.BlockSpec(memory_space=pltpu.HBM)
    vmem = pl.BlockSpec(memory_space=pltpu.VMEM)
    V = pltpu.VMEM
    S = pltpu.SemaphoreType.DMA
    shapes = ((rows, gl), (rows, half), (rows, gl), (1, rows), (ITERS, 2))
    args = (
        bus_of.reshape(-1, 128), dispatch, row(cost), row(p_low), row(p_high), row(ramp_limit), row(p_init),
        row(demand), ptdf, line_base, row(line_limit), line_dual, ramp_dual, row(balance_dual),
    )
    state = pl.pallas_call(
        functools.partial(kernel, (ntm, plane, gl_total, hours)),
        name="dispatch_step",
        out_shape=tuple(V(shape, F32) for shape in shapes),
        in_specs=[hbm] * len(args),
        out_specs=(vmem,) * len(shapes),
        scratch_shapes=[
            V((lines, buses), BF16),
            V((buses, lines // 128, 128), F32),
            V((128 * (lines // 128), 128), F32),
            V((2, gl, half), BF16),
            V((rows + 8, gl), F32),
            V((rows + 8, gl), F32),
            V((rows, gl), BF16),
            V((rows, half), F32),
            V((rows, half), F32),
            V((rows, half), F32),
            V((ITERS, 2, rows, half), jnp.int16),
            V((ITERS, 2, rows, half), BF16),
            V((rows, half), BF16),
            V((ITERS, 2, rows, half), jnp.int16),
            V((ITERS, 2, 2, 1, half), F32), V((ITERS, 2, 2, 1, half), F32),
            pltpu.SMEM((gl // 128, 128), jnp.int32),
            V((1, gl), F32), V((1, gl), F32), V((1, gl), F32), V((1, gl), F32), V((1, gl), F32),
            V((1, half), F32), V((1, half), F32), V((1, rows), F32), V((1, rows), F32),
            V((1, gl), F32), V((ITERS, 1, gl), F32), V((1, gl), F32), V((ITERS, 1, 128), F32), V((ITERS, 1, 128), F32),
            V((rows, 128), F32), V((rows, 128), F32), V((rows, 128), F32),
            V((2, 1, 128), F32), V((n_a, 1, 128), F32), V((nz, 1, 128), F32),
            S((12,)), S((2,)), S, S, S((5,)), S((5,)), S((ITERS, 4)), S((ITERS, 4)), S((ITERS, 4)), S((ITERS, 4)), S((ITERS,)), S((ITERS,)),
            S((4,)), S((4,)), S((2,)), S((2,)), S((2 * ITERS,)), S((2 * ITERS,)), S((2,)), S((2,)),
        ],
        compiler_params=pltpu.CompilerParams(
            collective_id=0, has_side_effects=True, vmem_limit_bytes=48 * 1024 * 1024
        ),
    )(*(pltpu.with_memory_space_constraint(a, pltpu.HBM) for a in args))
    x, y, mu, lam, mov = pl.pallas_call(
        write_out,
        name="write_out",
        out_shape=tuple(jax.ShapeDtypeStruct(shape, F32) for shape in shapes),
        in_specs=[vmem] * len(shapes),
        out_specs=(hbm,) * len(shapes),
        scratch_shapes=[S((len(shapes),))],
        compiler_params=pltpu.CompilerParams(vmem_limit_bytes=1024 * 1024),
    )(*(pltpu.with_memory_space_constraint(a, pltpu.VMEM) for a in state))
    return x, y, mu, lam.reshape(-1), mov


def solution(mesh):
    ntm = mesh.shape["tm"]
    plane = min(PLANE, ntm)

    def body(*args):
        return on_device(ntm, plane, args[0].shape[0] * ntm, args[0].shape[1] * mesh.shape["gen"], *args)

    in_specs = (
        P("tm", "gen"), P("gen"), P("gen"), P("gen"), P("gen"), P("gen"), P("tm"), P("gen"), P(),
        P("tm", "gen"), P("gen"), P("tm", "gen"), P("tm", "gen"), P("tm"),
    )
    out_specs = (P("tm", "gen"), P("tm", "gen"), P("tm", "gen"), P("tm"), P())
    return jax.shard_map(body, mesh=mesh, in_specs=in_specs, out_specs=out_specs, check_vma=False)
```

```python
import functools
import math

import jax
import jax.numpy as jnp
from jax import lax
from jax.experimental import pallas as pl
from jax.experimental.pallas import tpu as pltpu
from jax.sharding import PartitionSpec as P

TAU = 0.35
SIGMA = 0.35
ITERS = 2
PLANE = 16
MESH = pl.DeviceIdType.MESH
BF16 = jnp.bfloat16
F32 = jnp.float32
STEPS = 32767.0


def kernel(
    cfg,
    bus_h, x_h, cost_h, lo_h, hi_h, ramp_h, pinit_h, dem_h, ptdf_h, base_h, lim_h, y_h, mu_h, lam_h,
    xv, yo, muo, lam_o, mov_o,
    ptdf, table, stage, fac, muv, xbv, xbb, yv, yt, bt, flow, yb, ybs, frecv, scale, scale_x,
    bus, cost, lo, hi, ramp, pinit, lim, lim_x, dem, lam, mu_next, edge, xb_prev, xb_next, tot, tot_x,
    acc_p, acc_d, acc_t, msg, ar_a, ar_b,
    load_sem, ptdf_sem, yb_send, yb_recv, init_send, init_recv, f_send, f_recv, s_send, s_recv, t_send, t_recv,
    ys_send, ys_recv, yr_send, yr_recv, row_send, row_recv, ar_send, ar_recv,
):
    ntm, plane, gl_total, hours = cfg
    rows, gl = x_h.shape
    lines, buses = ptdf_h.shape
    half = lines // 2
    nz = ntm // plane
    w = 1.0 / math.sqrt(gl_total)
    cells = float(hours) * float(gl_total)
    tm = lax.axis_index("tm")
    gen = lax.axis_index("gen")
    other = 1 - gen
    partner = (tm, other)
    nxt = (lax.rem(tm + 1, ntm), gen)
    prv = (lax.rem(tm + ntm - 1, ntm), gen)
    twin = tm + 2 - 4 * lax.rem(tm // 2, 2)
    top = pl.ds(0, rows // 2)
    low = pl.ds(rows // 2, rows // 2)
    zz = tm // plane
    in_plane = lax.rem(tm, plane)
    n_a = 2 * plane
    mine_a = in_plane * 2 + gen

    def peer_a(d):
        q = lax.rem(mine_a + d, n_a)
        return (zz * plane + q // 2, lax.rem(q, 2))

    def peer_b(d):
        return (lax.rem(zz + d, nz) * plane + in_plane, gen)

    nblk = buses // 256
    n_load = min(4, nblk)
    per_load = nblk // n_load
    ptdf_copies = []
    for c in range(n_load):
        part = pl.ds(c * per_load * 256, per_load * 256)
        cp = pltpu.make_async_copy(ptdf_h.at[:, part], ptdf.at[:, part], ptdf_sem.at[c])
        cp.start()
        ptdf_copies.append(cp)
    loads = [
        pltpu.make_async_copy(s, d, load_sem.at[i])
        for i, (s, d) in enumerate(
            [
                (mu_h, muv.at[pl.ds(0, rows)]), (x_h, xv), (cost_h, cost), (y_h, yv),
                (lo_h, lo), (hi_h, hi), (ramp_h, ramp), (pinit_h, pinit), (lim_h, lim), (dem_h, dem),
                (lam_h, lam), (bus_h, bus),
            ]
        )
    ]
    for cp in loads[3:]:
        cp.start()

    barrier = pltpu.get_barrier_semaphore()

    def greet(dev):
        pl.semaphore_signal(barrier, inc=1, device_id=dev, device_id_type=MESH)

    greet(nxt)
    greet(prv)
    greet((twin, 0))
    greet((twin, 1))

    @pl.loop(1, n_a)
    def _(d):
        greet(peer_a(d))

    @pl.loop(1, nz)
    def _(d):
        greet(peer_b(d))

    nlb = lines // 128
    flat = table.reshape(buses * nlb, 128)
    for c in range(nblk):
        if c % per_load == 0:
            ptdf_copies[c // per_load].wait()
            if c // per_load == n_load - 1:
                for cp in loads[:3]:
                    cp.start()
        turned = ptdf[:, c * 256 : (c + 1) * 256].T.astype(F32)
        for j in range(nlb):
            flat[pl.ds(c * 256 * nlb + j, 256, stride=nlb), :] = turned[:, j * 128 : (j + 1) * 128]

    def send(src, dst, ssem, rsem, dev):
        return pltpu.make_async_remote_copy(
            src, dst, ssem, rsem, device_id=dev, device_id_type=MESH
        )

    def send_row(k, src, dst, dev):
        return pltpu.make_async_remote_copy(
            src, dst, row_send.at[k], row_recv.at[k], device_id=dev, device_id_type=MESH
        )

    group = 16
    n_group = 128 // group

    def gather(i):
        def fetch(s, k):
            stage[pl.ds((s * group + k) * nlb, nlb), :] = table[bus[i, s * group + k]]

        def pack(s, j):
            g0 = pl.multiple_of(i * 128 + s * group, group)
            got = stage[pl.ds(s * group * nlb + j, group, stride=nlb), :]
            fac[j // (nlb // 2), pl.ds(g0, group), pl.ds((j % (nlb // 2)) * 128, 128)] = got.astype(BF16)

        for k in range(group):
            fetch(0, k)
        for s in range(n_group):
            per = group // nlb
            for j in range(nlb):
                if s + 1 < n_group:
                    for k in range(per):
                        fetch(s + 1, j * per + k)
                pack(s, j)

    steps = gl // 128
    for cp in loads[3:]:
        cp.wait()
    pl.loop(0, steps // 8)(gather)
    yb[0, gen] = yv[...].astype(BF16)
    pl.semaphore_wait(barrier, n_a - 1 + nz - 1 + 4)

    yb_copy = send(yb.at[0, gen], yb.at[0, gen], yb_send, yb_recv, partner)
    yb_copy.start()
    mu_copy = send_row(0, mu_h.at[pl.ds(0, 1)], mu_next, prv)

    @pl.when(tm > 0)
    def _():
        mu_copy.start()

    pl.loop(steps // 8, steps // 2)(gather)
    moves = [
        send(src.at[part], dst.at[part], init_send.at[i], init_recv.at[i], (twin, dev))
        for i, (src, dst, part, dev) in enumerate(
            [(y_h, yt, top, gen), (y_h, yt, low, other), (base_h, bt, top, gen), (base_h, bt, low, other)]
        )
    ]
    moves.append(send(lim_h, lim_x, init_send.at[4], init_recv.at[4], (twin, other)))
    for cp in moves:
        cp.start()

    pl.loop(steps // 2, steps)(gather)
    for cp in loads[:3]:
        cp.wait()

    eye_r = lax.broadcasted_iota(jnp.int32, (rows, rows), 0) == lax.broadcasted_iota(
        jnp.int32, (rows, rows), 1
    )

    def to_column(row):
        return jnp.sum(jnp.where(eye_r, jnp.broadcast_to(row, (rows, rows)), 0.0), axis=1, keepdims=True)

    def to_row(col):
        return jnp.sum(jnp.where(eye_r, jnp.broadcast_to(col, (rows, rows)), 0.0), axis=0, keepdims=True)

    last = tm == ntm - 1
    first = tm == 0
    lam_col = to_column(lam[...])
    dem_col = to_column(dem[...])
    yb_copy.wait()

    @pl.when(tm > 0)
    def _():
        mu_copy.wait_send()

    @pl.when(tm < ntm - 1)
    def _():
        mu_copy.wait_recv()

    muv[pl.ds(rows, 1), :] = jnp.where(last, 0.0, mu_next[...])

    gc = 512
    sums = []
    for it in range(ITERS):
        acc_p[...] = jnp.zeros_like(acc_p)
        acc_d[...] = jnp.zeros_like(acc_d)
        acc_t[...] = jnp.zeros_like(acc_t)
        wlam = w * lam_col

        y_t = jnp.concatenate([yb[it, h].astype(F32).T.astype(BF16) for h in range(2)], axis=0)
        for c in range(gl // gc):
            sl = pl.ds(c * gc, gc)
            pulled_t = jnp.dot(fac[0, sl, :], y_t[:half], preferred_element_type=F32) + jnp.dot(
                fac[1, sl, :], y_t[half:], preferred_element_type=F32
            )
            pulled = pulled_t.T
            xc = xv[:, sl]
            grad = cost[:, sl] + wlam + pulled + muv[pl.ds(0, rows), sl] - muv[pl.ds(1, rows), sl]
            xn = jnp.clip(xc - TAU * grad, lo[:, sl], hi[:, sl])
            xb = 2.0 * xn - xc
            d = xn - xc
            d2 = d * d
            xv[:, sl] = xn
            xbv[pl.ds(8, rows), sl] = xb
            edge[it, 0, :, sl] = xb[rows - 1 :]
            if it < ITERS - 1:
                edge[it, 1, :, sl] = xb[:1]
            xbb[:, sl] = xb.astype(BF16)
            acc_p[...] += sum(d2[:, k * 128 : (k + 1) * 128] for k in range(gc // 128))
            acc_t[...] += sum(xb[:, k * 128 : (k + 1) * 128] for k in range(gc // 128))

        rows_out = [send_row(1 + 2 * it, edge.at[it, 0], xb_prev.at[it], nxt)]
        if it < ITERS - 1:
            rows_out.append(send_row(2 + 2 * it, edge.at[it, 1], xb_next, prv))
        has = [tm < ntm - 1, tm > 0]

        @pl.when(has[0])
        def _():
            rows_out[0].start()

        if it < ITERS - 1:

            @pl.when(has[1])
            def _():
                rows_out[1].start()

        tot_col = w * jnp.sum(acc_t[...], axis=1, keepdims=True)
        tot[it, :, pl.ds(0, rows)] = to_row(tot_col)
        t_copy = send(tot.at[it], tot_x.at[it], t_send.at[it], t_recv.at[it], partner)
        t_copy.start()
        f_copies = []
        for p in range(2):
            sums_p = jnp.dot(xbb[...], fac[p], preferred_element_type=F32)
            for r, part in enumerate((top, low)):
                block = sums_p[r * (rows // 2) : (r + 1) * (rows // 2)]
                largest = jnp.maximum(jnp.max(jnp.abs(block), axis=0, keepdims=True), 1e-30)
                flow[it, p, part] = jnp.round(block * (STEPS / largest)).astype(jnp.int32).astype(jnp.int16)
                scale[it, p, r] = largest * (1.0 / STEPS)
                dev = (twin, p if r == 0 else 1 - p)
                for cp in (
                    send(
                        scale.at[it, p, r], scale_x.at[it, gen, r], s_send.at[it, p * 2 + r],
                        s_recv.at[it, gen * 2 + r], dev,
                    ),
                    send(
                        flow.at[it, p, part], frecv.at[it, gen, part], f_send.at[it, p * 2 + r],
                        f_recv.at[it, gen * 2 + r], dev,
                    ),
                ):
                    cp.start()
                    f_copies.append(cp)
        def ramp_pass():
            @pl.when(has[0])
            def _():
                rows_out[0].wait_send()
                if it < ITERS - 1:
                    rows_out[1].wait_recv()

            @pl.when(has[1])
            def _():
                rows_out[0].wait_recv()
                if it < ITERS - 1:
                    rows_out[1].wait_send()

            xbv[pl.ds(7, 1), :] = jnp.where(first, pinit[...], xb_prev[it])
            if it < ITERS - 1:
                m_n = muv[pl.ds(rows, 1), :]
                u_n = m_n + SIGMA * (xb_next[...] - xbv[pl.ds(8 + rows - 1, 1), :])
                mn_n = u_n - jnp.clip(u_n, -SIGMA * ramp[...], SIGMA * ramp[...])
                muv[pl.ds(rows, 1), :] = jnp.where(last, 0.0, mn_n)

            @pl.loop(0, gl // gc)
            def _(c):
                sl = pl.ds(pl.multiple_of(c * gc, gc), gc)
                m = muv[pl.ds(0, rows), sl]
                u = m + SIGMA * (xbv[pl.ds(8, rows), sl] - xbv[pl.ds(7, rows), sl])
                r = SIGMA * ramp[:, sl]
                mn = u - jnp.clip(u, -r, r)
                if it < ITERS - 1:
                    muv[pl.ds(0, rows), sl] = mn
                else:
                    muo[:, sl] = mn
                d = mn - m
                d2 = d * d
                acc_d[...] += sum(d2[:, k * 128 : (k + 1) * 128] for k in range(gc // 128))

        if it == ITERS - 1:
            ramp_pass()
        t_copy.wait()
        totals = tot_col + to_column(tot_x[it, :, pl.ds(0, rows)])
        lam_new = lam_col + SIGMA * (totals - dem_col)
        dl = lam_new - lam_col
        lam_col = lam_new

        for cp in f_copies:
            cp.wait_send()
        for s in range(2):
            for r, part in enumerate((top, low)):
                send(
                    scale.at[it, 0, r], scale_x.at[it, s, r], s_send.at[it, r],
                    s_recv.at[it, s * 2 + r], (twin, s),
                ).wait_recv()
                send(
                    flow.at[it, 0, part], frecv.at[it, s, part], f_send.at[it, r],
                    f_recv.at[it, s * 2 + r], (twin, s),
                ).wait_recv()
        if it == 0:
            for cp in moves:
                cp.wait()
        half_rows = rows // 2
        for r, part in enumerate((top, low)):
            old = yt[part, :]
            v = old + SIGMA * sum(
                frecv[it, s, part, :].astype(jnp.int32).astype(F32) * scale_x[it, s, r] for s in range(2)
            )
            bv = bt[part, :]
            lv = (lim if r == 0 else lim_x)[...]
            yn = v - jnp.clip(v, SIGMA * (bv - lv), SIGMA * (bv + lv))
            yt[part, :] = yn
            if it < ITERS - 1:
                ybs[part, :] = yn.astype(BF16)
                for dev in range(2):
                    send(
                        ybs.at[part], yb.at[it + 1, gen if r == 0 else other, part],
                        ys_send.at[dev * 2 + r], ys_recv.at[gen * 2 + r], (twin, dev),
                    ).start()
            dy = yn - old
            dy2 = dy * dy
            acc_d[pl.ds(r * half_rows, half_rows), :] += sum(
                dy2[:, k * 128 : (k + 1) * 128] for k in range(half // 128)
            )
        if it < ITERS - 1:
            ramp_pass()
        primal = jnp.sum(acc_p[...], keepdims=True) / (TAU * cells)
        dual = (
            jnp.sum(acc_d[...], keepdims=True)
            + jnp.where(gen == 0, jnp.sum(dl * dl, keepdims=True), 0.0)
        ) / (SIGMA * cells)
        sums += [primal, dual]
        if it < ITERS - 1:
            for s in range(2):
                for r, part in enumerate((top, low)):
                    piece = s if r == 0 else 1 - s
                    send(
                        ybs.at[part], yb.at[it + 1, piece, part], ys_send.at[s * 2 + r],
                        ys_recv.at[s * 2 + r], (twin, s),
                    ).wait()

    lane = lax.broadcasted_iota(jnp.int32, (1, 128), 1)
    packed = jnp.zeros((1, 128), F32)
    for k, s in enumerate(sums):
        packed = jnp.where(lane == k, s, packed)

    def all_sum(value, buf, k, n, mine, peer, between=None):
        msg[k] = value
        buf[mine] = value

        @pl.loop(1, n)
        def _(d):
            pltpu.make_async_remote_copy(
                msg.at[k], buf.at[mine], ar_send.at[k], ar_recv.at[k],
                device_id=peer(d), device_id_type=MESH,
            ).start()

        if between is not None:
            between()
        several = buf.at[pl.ds(0, n - 1)]
        pltpu.make_async_copy(several, several, ar_send.at[k]).wait()
        pltpu.make_async_copy(several, several, ar_recv.at[k]).wait()
        return jnp.sum(buf[...], axis=0)

    y_back = [
        send(yt.at[part], yo.at[part], yr_send.at[r], yr_recv.at[r], (twin, dev))
        for r, (part, dev) in enumerate(((top, gen), (low, other)))
    ]

    def return_y():
        for cp in y_back:
            cp.start()

    total = all_sum(packed, ar_a, 0, n_a, mine_a, peer_a, return_y)
    total = all_sum(total, ar_b, 1, nz, zz, peer_b)
    place = 2 * lax.broadcasted_iota(jnp.int32, (ITERS, 2), 0) + lax.broadcasted_iota(
        jnp.int32, (ITERS, 2), 1
    )
    result = jnp.zeros((ITERS, 2), F32)
    for k in range(2 * ITERS):
        one = jnp.sum(jnp.where(lane == k, total, 0.0), axis=1, keepdims=True)
        result = jnp.where(place == k, one, result)
    mov_o[...] = result
    lam_o[...] = to_row(lam_col)
    for cp in y_back:
        cp.wait()


def write_out(x, y, mu, lam, mov, x_h, y_h, mu_h, lam_h, mov_h, sem):
    copies = [
        pltpu.make_async_copy(s, d, sem.at[i])
        for i, (s, d) in enumerate(((x, x_h), (mu, mu_h), (y, y_h), (lam, lam_h), (mov, mov_h)))
    ]
    for cp in copies:
        cp.start()
    for cp in copies:
        cp.wait()


def on_device(ntm, plane, hours, gl_total,
              dispatch, cost, p_low, p_high, ramp_limit, p_init, demand, bus_of, ptdf, line_base,
              line_limit, line_dual, ramp_dual, balance_dual):
    rows, gl = dispatch.shape
    lines, buses = ptdf.shape
    half = lines // 2
    n_a = 2 * plane
    nz = ntm // plane
    row = lambda a: a.reshape(1, -1)
    hbm = pl.BlockSpec(memory_space=pltpu.HBM)
    vmem = pl.BlockSpec(memory_space=pltpu.VMEM)
    V = pltpu.VMEM
    S = pltpu.SemaphoreType.DMA
    shapes = ((rows, gl), (rows, half), (rows, gl), (1, rows), (ITERS, 2))
    args = (
        bus_of.reshape(-1, 128), dispatch, row(cost), row(p_low), row(p_high), row(ramp_limit), row(p_init),
        row(demand), ptdf, line_base, row(line_limit), line_dual, ramp_dual, row(balance_dual),
    )
    state = pl.pallas_call(
        functools.partial(kernel, (ntm, plane, gl_total, hours)),
        name="dispatch_step",
        out_shape=tuple(V(shape, F32) for shape in shapes),
        in_specs=[hbm] * len(args),
        out_specs=(vmem,) * len(shapes),
        scratch_shapes=[
            V((lines, buses), BF16),
            V((buses, lines // 128, 128), F32),
            V((128 * (lines // 128), 128), F32),
            V((2, gl, half), BF16),
            V((rows + 8, gl), F32),
            V((rows + 8, gl), F32),
            V((rows, gl), BF16),
            V((rows, half), F32),
            V((rows, half), F32),
            V((rows, half), F32),
            V((ITERS, 2, rows, half), jnp.int16),
            V((ITERS, 2, rows, half), BF16),
            V((rows, half), BF16),
            V((ITERS, 2, rows, half), jnp.int16),
            V((ITERS, 2, 2, 1, half), F32), V((ITERS, 2, 2, 1, half), F32),
            pltpu.SMEM((gl // 128, 128), jnp.int32),
            V((1, gl), F32), V((1, gl), F32), V((1, gl), F32), V((1, gl), F32), V((1, gl), F32),
            V((1, half), F32), V((1, half), F32), V((1, rows), F32), V((1, rows), F32),
            V((1, gl), F32), V((ITERS, 2, 1, gl), F32), V((ITERS, 1, gl), F32), V((1, gl), F32), V((ITERS, 1, 128), F32), V((ITERS, 1, 128), F32),
            V((rows, 128), F32), V((rows, 128), F32), V((rows, 128), F32),
            V((2, 1, 128), F32), V((n_a, 1, 128), F32), V((nz, 1, 128), F32),
            S((12,)), S((4,)), S, S, S((5,)), S((5,)), S((ITERS, 4)), S((ITERS, 4)), S((ITERS, 4)), S((ITERS, 4)), S((ITERS,)), S((ITERS,)),
            S((4,)), S((4,)), S((2,)), S((2,)), S((2 * ITERS,)), S((2 * ITERS,)), S((2,)), S((2,)),
        ],
        compiler_params=pltpu.CompilerParams(
            collective_id=0, has_side_effects=True, vmem_limit_bytes=48 * 1024 * 1024
        ),
    )(*(pltpu.with_memory_space_constraint(a, pltpu.HBM) for a in args))
    x, y, mu, lam, mov = pl.pallas_call(
        write_out,
        name="write_out",
        out_shape=tuple(jax.ShapeDtypeStruct(shape, F32) for shape in shapes),
        in_specs=[vmem] * len(shapes),
        out_specs=(hbm,) * len(shapes),
        scratch_shapes=[S((len(shapes),))],
        compiler_params=pltpu.CompilerParams(vmem_limit_bytes=1024 * 1024),
    )(*(pltpu.with_memory_space_constraint(a, pltpu.VMEM) for a in state))
    return x, y, mu, lam.reshape(-1), mov


def solution(mesh):
    ntm = mesh.shape["tm"]
    plane = min(PLANE, ntm)

    def body(*args):
        return on_device(ntm, plane, args[0].shape[0] * ntm, args[0].shape[1] * mesh.shape["gen"], *args)

    in_specs = (
        P("tm", "gen"), P("gen"), P("gen"), P("gen"), P("gen"), P("gen"), P("tm"), P("gen"), P(),
        P("tm", "gen"), P("gen"), P("tm", "gen"), P("tm", "gen"), P("tm"),
    )
    out_specs = (P("tm", "gen"), P("tm", "gen"), P("tm", "gen"), P("tm"), P())
    return jax.shard_map(body, mesh=mesh, in_specs=in_specs, out_specs=out_specs, check_vma=False)
```

```python
import functools
import math

import jax
import jax.numpy as jnp
from jax import lax
from jax.experimental import pallas as pl
from jax.experimental.pallas import tpu as pltpu
from jax.sharding import PartitionSpec as P

TAU = 0.35
SIGMA = 0.35
ITERS = 2
PLANE = 16
MESH = pl.DeviceIdType.MESH
BF16 = jnp.bfloat16
F32 = jnp.float32
STEPS = 32767.0


def kernel(
    cfg,
    bus_h, x_h, cost_h, lo_h, hi_h, ramp_h, pinit_h, dem_h, ptdf_h, base_h, lim_h, y_h, mu_h, lam_h,
    xv, yo, muo, lam_o, mov_o,
    ptdf, table, stage, fac, muv, xbv, xbb, yv, yt, bt, flow, yb, ybs, frecv, scale, scale_x,
    bus, cost, lo, hi, ramp, pinit, lim, lim_x, lims, dem, lam, mu_next, edge, xb_prev, xb_next, tot, tot_x,
    acc_p, acc_d, acc_t, msg, ar_a, ar_b,
    load_sem, ptdf_sem, yb_send, yb_recv, init_send, init_recv, f_send, f_recv, s_send, s_recv, t_send, t_recv,
    ys_send, ys_recv, yr_send, yr_recv, row_send, row_recv, ar_send, ar_recv,
):
    ntm, plane, gl_total, hours = cfg
    rows, gl = x_h.shape
    lines, buses = ptdf_h.shape
    half = lines // 2
    nz = ntm // plane
    w = 1.0 / math.sqrt(gl_total)
    cells = float(hours) * float(gl_total)
    tm = lax.axis_index("tm")
    gen = lax.axis_index("gen")
    other = 1 - gen
    partner = (tm, other)
    nxt = (lax.rem(tm + 1, ntm), gen)
    prv = (lax.rem(tm + ntm - 1, ntm), gen)
    twin = tm + 2 - 4 * lax.rem(tm // 2, 2)
    top = pl.ds(0, rows // 2)
    low = pl.ds(rows // 2, rows // 2)
    zz = tm // plane
    in_plane = lax.rem(tm, plane)
    n_a = 2 * plane
    mine_a = in_plane * 2 + gen

    def peer_a(d):
        q = lax.rem(mine_a + d, n_a)
        return (zz * plane + q // 2, lax.rem(q, 2))

    def peer_b(d):
        return (lax.rem(zz + d, nz) * plane + in_plane, gen)

    nblk = buses // 256
    n_load = min(4, nblk)
    per_load = nblk // n_load
    ptdf_copies = []
    for c in range(n_load):
        part = pl.ds(c * per_load * 256, per_load * 256)
        cp = pltpu.make_async_copy(ptdf_h.at[:, part], ptdf.at[:, part], ptdf_sem.at[c])
        cp.start()
        ptdf_copies.append(cp)
    loads = [
        pltpu.make_async_copy(s, d, load_sem.at[i])
        for i, (s, d) in enumerate(
            [
                (mu_h, muv.at[pl.ds(0, rows)]), (x_h, xv), (cost_h, cost), (y_h, yv),
                (lo_h, lo), (hi_h, hi), (ramp_h, ramp), (pinit_h, pinit), (lim_h, lim), (dem_h, dem),
                (lam_h, lam), (bus_h, bus),
            ]
        )
    ]
    for cp in loads[3:]:
        cp.start()

    barrier = pltpu.get_barrier_semaphore()

    def greet(dev):
        pl.semaphore_signal(barrier, inc=1, device_id=dev, device_id_type=MESH)

    greet(nxt)
    greet(prv)
    greet((twin, 0))
    greet((twin, 1))

    @pl.loop(1, n_a)
    def _(d):
        greet(peer_a(d))

    @pl.loop(1, nz)
    def _(d):
        greet(peer_b(d))

    nlb = lines // 128
    flat = table.reshape(buses * nlb, 128)
    for c in range(nblk):
        if c % per_load == 0:
            ptdf_copies[c // per_load].wait()
            if c // per_load == n_load - 1:
                for cp in loads[:3]:
                    cp.start()
        turned = ptdf[:, c * 256 : (c + 1) * 256].T.astype(F32)
        for j in range(nlb):
            flat[pl.ds(c * 256 * nlb + j, 256, stride=nlb), :] = turned[:, j * 128 : (j + 1) * 128]

    def send(src, dst, ssem, rsem, dev):
        return pltpu.make_async_remote_copy(
            src, dst, ssem, rsem, device_id=dev, device_id_type=MESH
        )

    def send_row(k, src, dst, dev):
        return pltpu.make_async_remote_copy(
            src, dst, row_send.at[k], row_recv.at[k], device_id=dev, device_id_type=MESH
        )

    group = 16
    n_group = 128 // group

    def gather(i):
        def fetch(s, k):
            stage[pl.ds((s * group + k) * nlb, nlb), :] = table[bus[i, s * group + k]]

        def pack(s, j):
            g0 = pl.multiple_of(i * 128 + s * group, group)
            got = stage[pl.ds(s * group * nlb + j, group, stride=nlb), :]
            fac[j // (nlb // 2), pl.ds(g0, group), pl.ds((j % (nlb // 2)) * 128, 128)] = got.astype(BF16)

        for k in range(group):
            fetch(0, k)
        for s in range(n_group):
            per = group // nlb
            for j in range(nlb):
                if s + 1 < n_group:
                    for k in range(per):
                        fetch(s + 1, j * per + k)
                pack(s, j)

    steps = gl // 128
    for cp in loads[3:]:
        cp.wait()
    pl.loop(0, steps // 8)(gather)
    yb[0, gen] = yv[...].astype(BF16)
    pl.semaphore_wait(barrier, n_a - 1 + nz - 1 + 4)

    yb_copy = send(yb.at[0, gen], yb.at[0, gen], yb_send, yb_recv, partner)
    yb_copy.start()
    mu_copy = send_row(0, mu_h.at[pl.ds(0, 1)], mu_next, prv)

    @pl.when(tm > 0)
    def _():
        mu_copy.start()

    pl.loop(steps // 8, steps // 2)(gather)
    moves = [
        send(src.at[part], dst.at[part], init_send.at[i], init_recv.at[i], (twin, dev))
        for i, (src, dst, part, dev) in enumerate(
            [(y_h, yt, top, gen), (y_h, yt, low, other), (base_h, bt, top, gen), (base_h, bt, low, other)]
        )
    ]
    moves.append(send(lim_h, lim_x, init_send.at[4], init_recv.at[4], (twin, other)))
    for cp in moves:
        cp.start()

    pl.loop(steps // 2, steps)(gather)
    for cp in loads[:3]:
        cp.wait()

    eye_r = lax.broadcasted_iota(jnp.int32, (rows, rows), 0) == lax.broadcasted_iota(
        jnp.int32, (rows, rows), 1
    )

    def to_column(row):
        return jnp.sum(jnp.where(eye_r, jnp.broadcast_to(row, (rows, rows)), 0.0), axis=1, keepdims=True)

    def to_row(col):
        return jnp.sum(jnp.where(eye_r, jnp.broadcast_to(col, (rows, rows)), 0.0), axis=0, keepdims=True)

    last = tm == ntm - 1
    first = tm == 0
    lam_col = to_column(lam[...])
    dem_col = to_column(dem[...])
    yb_copy.wait()

    @pl.when(tm > 0)
    def _():
        mu_copy.wait_send()

    @pl.when(tm < ntm - 1)
    def _():
        mu_copy.wait_recv()

    muv[pl.ds(rows, 1), :] = jnp.where(last, 0.0, mu_next[...])

    gc = 512
    sums = []
    for it in range(ITERS):
        acc_p[...] = jnp.zeros_like(acc_p)
        acc_d[...] = jnp.zeros_like(acc_d)
        acc_t[...] = jnp.zeros_like(acc_t)
        wlam = w * lam_col

        y_t = jnp.concatenate([yb[it, h].astype(F32).T.astype(BF16) for h in range(2)], axis=0)
        for c in range(gl // gc):
            sl = pl.ds(c * gc, gc)
            pulled_t = jnp.dot(fac[0, sl, :], y_t[:half], preferred_element_type=F32) + jnp.dot(
                fac[1, sl, :], y_t[half:], preferred_element_type=F32
            )
            pulled = pulled_t.T
            xc = xv[:, sl]
            grad = cost[:, sl] + wlam + pulled + muv[pl.ds(0, rows), sl] - muv[pl.ds(1, rows), sl]
            xn = jnp.clip(xc - TAU * grad, lo[:, sl], hi[:, sl])
            xb = 2.0 * xn - xc
            d = xn - xc
            d2 = d * d
            xv[:, sl] = xn
            xbv[pl.ds(8, rows), sl] = xb
            edge[it, 0, :, sl] = xb[rows - 1 :]
            if it < ITERS - 1:
                edge[it, 1, :, sl] = xb[:1]
            xbb[:, sl] = xb.astype(BF16)
            acc_p[...] += sum(d2[:, k * 128 : (k + 1) * 128] for k in range(gc // 128))
            acc_t[...] += sum(xb[:, k * 128 : (k + 1) * 128] for k in range(gc // 128))

        rows_out = [send_row(1 + 2 * it, edge.at[it, 0], xb_prev.at[it], nxt)]
        if it < ITERS - 1:
            rows_out.append(send_row(2 + 2 * it, edge.at[it, 1], xb_next, prv))
        has = [tm < ntm - 1, tm > 0]

        @pl.when(has[0])
        def _():
            rows_out[0].start()

        if it < ITERS - 1:

            @pl.when(has[1])
            def _():
                rows_out[1].start()

        tot_col = w * jnp.sum(acc_t[...], axis=1, keepdims=True)
        tot[it, :, pl.ds(0, rows)] = to_row(tot_col)
        t_copy = send(tot.at[it], tot_x.at[it], t_send.at[it], t_recv.at[it], partner)
        t_copy.start()
        f_copies = []
        for p in range(2):
            sums_p = jnp.dot(xbb[...], fac[p], preferred_element_type=F32)
            for r, part in enumerate((top, low)):
                block = sums_p[r * (rows // 2) : (r + 1) * (rows // 2)]
                largest = jnp.maximum(jnp.max(jnp.abs(block), axis=0, keepdims=True), 1e-30)
                flow[it, p, part] = jnp.round(block * (STEPS / largest)).astype(jnp.int32).astype(jnp.int16)
                scale[it, p, r] = largest * (1.0 / STEPS)
                dev = (twin, p if r == 0 else 1 - p)
                for cp in (
                    send(
                        scale.at[it, p, r], scale_x.at[it, gen, r], s_send.at[it, p * 2 + r],
                        s_recv.at[it, gen * 2 + p], dev,
                    ),
                    send(
                        flow.at[it, p, part], frecv.at[it, gen, part], f_send.at[it, p * 2 + r],
                        f_recv.at[it, gen * 2 + p], dev,
                    ),
                ):
                    cp.start()
                    f_copies.append(cp)
        def ramp_pass():
            @pl.when(has[0])
            def _():
                rows_out[0].wait_send()
                if it < ITERS - 1:
                    rows_out[1].wait_recv()

            @pl.when(has[1])
            def _():
                rows_out[0].wait_recv()
                if it < ITERS - 1:
                    rows_out[1].wait_send()

            xbv[pl.ds(7, 1), :] = jnp.where(first, pinit[...], xb_prev[it])
            if it < ITERS - 1:
                m_n = muv[pl.ds(rows, 1), :]
                u_n = m_n + SIGMA * (xb_next[...] - xbv[pl.ds(8 + rows - 1, 1), :])
                mn_n = u_n - jnp.clip(u_n, -SIGMA * ramp[...], SIGMA * ramp[...])
                muv[pl.ds(rows, 1), :] = jnp.where(last, 0.0, mn_n)

            @pl.loop(0, gl // gc)
            def _(c):
                sl = pl.ds(pl.multiple_of(c * gc, gc), gc)
                m = muv[pl.ds(0, rows), sl]
                u = m + SIGMA * (xbv[pl.ds(8, rows), sl] - xbv[pl.ds(7, rows), sl])
                r = SIGMA * ramp[:, sl]
                mn = u - jnp.clip(u, -r, r)
                if it < ITERS - 1:
                    muv[pl.ds(0, rows), sl] = mn
                else:
                    muo[:, sl] = mn
                d = mn - m
                d2 = d * d
                acc_d[...] += sum(d2[:, k * 128 : (k + 1) * 128] for k in range(gc // 128))

        if it == ITERS - 1:
            ramp_pass()
        t_copy.wait()
        totals = tot_col + to_column(tot_x[it, :, pl.ds(0, rows)])
        lam_new = lam_col + SIGMA * (totals - dem_col)
        dl = lam_new - lam_col
        lam_col = lam_new

        for cp in f_copies:
            cp.wait_send()
        if it == 0:
            for cp in moves:
                cp.wait()
            lims[other] = lim_x[...]
            lims[gen] = lim[...]
        half_rows = rows // 2
        for p in range(2):
            r = gen if p == 0 else other
            part = pl.ds(pl.multiple_of(r * half_rows, half_rows), half_rows)
            for s in range(2):
                send(
                    scale.at[it, 0, 0], scale_x.at[it, s, r], s_send.at[it, 0], s_recv.at[it, s * 2 + p],
                    (twin, s),
                ).wait_recv()
                send(
                    flow.at[it, 0, top], frecv.at[it, s, part], f_send.at[it, 0], f_recv.at[it, s * 2 + p],
                    (twin, s),
                ).wait_recv()
            old = yt[part, :]
            v = old + SIGMA * sum(
                frecv[it, s, part, :].astype(jnp.int32).astype(F32) * scale_x[it, s, r] for s in range(2)
            )
            bv = bt[part, :]
            lv = lims[p]
            yn = v - jnp.clip(v, SIGMA * (bv - lv), SIGMA * (bv + lv))
            yt[part, :] = yn
            if it < ITERS - 1:
                ybs[part, :] = yn.astype(BF16)
                for dev in range(2):
                    send(
                        ybs.at[part], yb.at[it + 1, p, part], ys_send.at[dev * 2 + p],
                        ys_recv.at[gen * 2 + p], (twin, dev),
                    ).start()
            dy = yn - old
            dy2 = dy * dy
            acc_d[pl.ds(0, half_rows), :] += sum(
                dy2[:, k * 128 : (k + 1) * 128] for k in range(half // 128)
            )
        if it < ITERS - 1:
            ramp_pass()
        primal = jnp.sum(acc_p[...], keepdims=True) / (TAU * cells)
        dual = (
            jnp.sum(acc_d[...], keepdims=True)
            + jnp.where(gen == 0, jnp.sum(dl * dl, keepdims=True), 0.0)
        ) / (SIGMA * cells)
        sums += [primal, dual]
        if it < ITERS - 1:
            for s in range(2):
                for p in range(2):
                    part = top if s == p else low
                    send(
                        ybs.at[part], yb.at[it + 1, p, part], ys_send.at[s * 2 + p],
                        ys_recv.at[s * 2 + p], (twin, s),
                    ).wait()

    lane = lax.broadcasted_iota(jnp.int32, (1, 128), 1)
    packed = jnp.zeros((1, 128), F32)
    for k, s in enumerate(sums):
        packed = jnp.where(lane == k, s, packed)

    def all_sum(value, buf, k, n, mine, peer, between=None):
        msg[k] = value
        buf[mine] = value

        @pl.loop(1, n)
        def _(d):
            pltpu.make_async_remote_copy(
                msg.at[k], buf.at[mine], ar_send.at[k], ar_recv.at[k],
                device_id=peer(d), device_id_type=MESH,
            ).start()

        if between is not None:
            between()
        several = buf.at[pl.ds(0, n - 1)]
        pltpu.make_async_copy(several, several, ar_send.at[k]).wait()
        pltpu.make_async_copy(several, several, ar_recv.at[k]).wait()
        return jnp.sum(buf[...], axis=0)

    y_back = [
        send(yt.at[part], yo.at[part], yr_send.at[r], yr_recv.at[r], (twin, dev))
        for r, (part, dev) in enumerate(((top, gen), (low, other)))
    ]

    def return_y():
        for cp in y_back:
            cp.start()

    total = all_sum(packed, ar_a, 0, n_a, mine_a, peer_a, return_y)
    total = all_sum(total, ar_b, 1, nz, zz, peer_b)
    place = 2 * lax.broadcasted_iota(jnp.int32, (ITERS, 2), 0) + lax.broadcasted_iota(
        jnp.int32, (ITERS, 2), 1
    )
    result = jnp.zeros((ITERS, 2), F32)
    for k in range(2 * ITERS):
        one = jnp.sum(jnp.where(lane == k, total, 0.0), axis=1, keepdims=True)
        result = jnp.where(place == k, one, result)
    mov_o[...] = result
    lam_o[...] = to_row(lam_col)
    for cp in y_back:
        cp.wait()


def write_out(x, y, mu, lam, mov, x_h, y_h, mu_h, lam_h, mov_h, sem):
    copies = [
        pltpu.make_async_copy(s, d, sem.at[i])
        for i, (s, d) in enumerate(((x, x_h), (mu, mu_h), (y, y_h), (lam, lam_h), (mov, mov_h)))
    ]
    for cp in copies:
        cp.start()
    for cp in copies:
        cp.wait()


def on_device(ntm, plane, hours, gl_total,
              dispatch, cost, p_low, p_high, ramp_limit, p_init, demand, bus_of, ptdf, line_base,
              line_limit, line_dual, ramp_dual, balance_dual):
    rows, gl = dispatch.shape
    lines, buses = ptdf.shape
    half = lines // 2
    n_a = 2 * plane
    nz = ntm // plane
    row = lambda a: a.reshape(1, -1)
    hbm = pl.BlockSpec(memory_space=pltpu.HBM)
    vmem = pl.BlockSpec(memory_space=pltpu.VMEM)
    V = pltpu.VMEM
    S = pltpu.SemaphoreType.DMA
    shapes = ((rows, gl), (rows, half), (rows, gl), (1, rows), (ITERS, 2))
    args = (
        bus_of.reshape(-1, 128), dispatch, row(cost), row(p_low), row(p_high), row(ramp_limit), row(p_init),
        row(demand), ptdf, line_base, row(line_limit), line_dual, ramp_dual, row(balance_dual),
    )
    state = pl.pallas_call(
        functools.partial(kernel, (ntm, plane, gl_total, hours)),
        name="dispatch_step",
        out_shape=tuple(V(shape, F32) for shape in shapes),
        in_specs=[hbm] * len(args),
        out_specs=(vmem,) * len(shapes),
        scratch_shapes=[
            V((lines, buses), BF16),
            V((buses, lines // 128, 128), F32),
            V((128 * (lines // 128), 128), F32),
            V((2, gl, half), BF16),
            V((rows + 8, gl), F32),
            V((rows + 8, gl), F32),
            V((rows, gl), BF16),
            V((rows, half), F32),
            V((rows, half), F32),
            V((rows, half), F32),
            V((ITERS, 2, rows, half), jnp.int16),
            V((ITERS, 2, rows, half), BF16),
            V((rows, half), BF16),
            V((ITERS, 2, rows, half), jnp.int16),
            V((ITERS, 2, 2, 1, half), F32), V((ITERS, 2, 2, 1, half), F32),
            pltpu.SMEM((gl // 128, 128), jnp.int32),
            V((1, gl), F32), V((1, gl), F32), V((1, gl), F32), V((1, gl), F32), V((1, gl), F32),
            V((1, half), F32), V((1, half), F32), V((2, 1, half), F32), V((1, rows), F32), V((1, rows), F32),
            V((1, gl), F32), V((ITERS, 2, 1, gl), F32), V((ITERS, 1, gl), F32), V((1, gl), F32), V((ITERS, 1, 128), F32), V((ITERS, 1, 128), F32),
            V((rows, 128), F32), V((rows, 128), F32), V((rows, 128), F32),
            V((2, 1, 128), F32), V((n_a, 1, 128), F32), V((nz, 1, 128), F32),
            S((12,)), S((4,)), S, S, S((5,)), S((5,)), S((ITERS, 4)), S((ITERS, 4)), S((ITERS, 4)), S((ITERS, 4)), S((ITERS,)), S((ITERS,)),
            S((4,)), S((4,)), S((2,)), S((2,)), S((2 * ITERS,)), S((2 * ITERS,)), S((2,)), S((2,)),
        ],
        compiler_params=pltpu.CompilerParams(
            collective_id=0, has_side_effects=True, vmem_limit_bytes=48 * 1024 * 1024
        ),
    )(*(pltpu.with_memory_space_constraint(a, pltpu.HBM) for a in args))
    x, y, mu, lam, mov = pl.pallas_call(
        write_out,
        name="write_out",
        out_shape=tuple(jax.ShapeDtypeStruct(shape, F32) for shape in shapes),
        in_specs=[vmem] * len(shapes),
        out_specs=(hbm,) * len(shapes),
        scratch_shapes=[S((len(shapes),))],
        compiler_params=pltpu.CompilerParams(vmem_limit_bytes=1024 * 1024),
    )(*(pltpu.with_memory_space_constraint(a, pltpu.VMEM) for a in state))
    return x, y, mu, lam.reshape(-1), mov


def solution(mesh):
    ntm = mesh.shape["tm"]
    plane = min(PLANE, ntm)

    def body(*args):
        return on_device(ntm, plane, args[0].shape[0] * ntm, args[0].shape[1] * mesh.shape["gen"], *args)

    in_specs = (
        P("tm", "gen"), P("gen"), P("gen"), P("gen"), P("gen"), P("gen"), P("tm"), P("gen"), P(),
        P("tm", "gen"), P("gen"), P("tm", "gen"), P("tm", "gen"), P("tm"),
    )
    out_specs = (P("tm", "gen"), P("tm", "gen"), P("tm", "gen"), P("tm"), P())
    return jax.shard_map(body, mesh=mesh, in_specs=in_specs, out_specs=out_specs, check_vma=False)
```

```python
import functools
import math

import jax
import jax.numpy as jnp
from jax import lax
from jax.experimental import pallas as pl
from jax.experimental.pallas import tpu as pltpu
from jax.sharding import PartitionSpec as P

TAU = 0.35
SIGMA = 0.35
ITERS = 2
PLANE = 16
MESH = pl.DeviceIdType.MESH
BF16 = jnp.bfloat16
F32 = jnp.float32
STEPS = 32767.0


def kernel(
    cfg,
    bus_h, x_h, cost_h, lo_h, hi_h, ramp_h, pinit_h, dem_h, ptdf_h, base_h, lim_h, y_h, mu_h, lam_h,
    xv, yo, muo, lam_o, mov_o,
    ptdf, table, stage, fac, muv, xbv, xbb, yv, yt, bt, flow, yb, ybs, frecv, scale, scale_x,
    bus, cost, lo, hi, ramp, pinit, lim, lim_x, lims, dem, lam, mu_next, edge, xb_prev, xb_next, tot, tot_x,
    acc_p, acc_d, acc_t, msg, ar_a, ar_b,
    load_sem, ptdf_sem, yb_send, yb_recv, init_send, init_recv, f_send, f_recv, s_send, s_recv, t_send, t_recv,
    ys_send, ys_recv, yr_send, yr_recv, row_send, row_recv, ar_send, ar_recv,
):
    ntm, plane, gl_total, hours = cfg
    rows, gl = x_h.shape
    lines, buses = ptdf_h.shape
    half = lines // 2
    nz = ntm // plane
    w = 1.0 / math.sqrt(gl_total)
    cells = float(hours) * float(gl_total)
    tm = lax.axis_index("tm")
    gen = lax.axis_index("gen")
    other = 1 - gen
    partner = (tm, other)
    nxt = (lax.rem(tm + 1, ntm), gen)
    prv = (lax.rem(tm + ntm - 1, ntm), gen)
    twin = tm + 2 - 4 * lax.rem(tm // 2, 2)
    top = pl.ds(0, rows // 2)
    low = pl.ds(rows // 2, rows // 2)
    zz = tm // plane
    in_plane = lax.rem(tm, plane)
    n_a = 2 * plane
    mine_a = in_plane * 2 + gen

    def peer_a(d):
        q = lax.rem(mine_a + d, n_a)
        return (zz * plane + q // 2, lax.rem(q, 2))

    def peer_b(d):
        return (lax.rem(zz + d, nz) * plane + in_plane, gen)

    nblk = buses // 256
    n_load = min(4, nblk)
    per_load = nblk // n_load
    ptdf_copies = []
    for c in range(n_load):
        part = pl.ds(c * per_load * 256, per_load * 256)
        cp = pltpu.make_async_copy(ptdf_h.at[:, part], ptdf.at[:, part], ptdf_sem.at[c])
        cp.start()
        ptdf_copies.append(cp)
    loads = [
        pltpu.make_async_copy(s, d, load_sem.at[i])
        for i, (s, d) in enumerate(
            [
                (mu_h, muv.at[pl.ds(0, rows)]), (x_h, xv), (cost_h, cost), (y_h, yv),
                (lo_h, lo), (hi_h, hi), (ramp_h, ramp), (pinit_h, pinit), (lim_h, lim), (dem_h, dem),
                (lam_h, lam), (bus_h, bus),
            ]
        )
    ]
    for cp in loads[3:]:
        cp.start()

    barrier = pltpu.get_barrier_semaphore()

    def greet(dev):
        pl.semaphore_signal(barrier, inc=1, device_id=dev, device_id_type=MESH)

    greet(nxt)
    greet(prv)
    greet((twin, 0))
    greet((twin, 1))

    @pl.loop(1, n_a)
    def _(d):
        greet(peer_a(d))

    @pl.loop(1, nz)
    def _(d):
        greet(peer_b(d))

    nlb = lines // 128
    flat = table.reshape(buses * nlb, 128)
    for c in range(nblk):
        if c % per_load == 0:
            ptdf_copies[c // per_load].wait()
            if c // per_load == n_load - 1:
                for cp in loads[:3]:
                    cp.start()
        turned = ptdf[:, c * 256 : (c + 1) * 256].T.astype(F32)
        for j in range(nlb):
            flat[pl.ds(c * 256 * nlb + j, 256, stride=nlb), :] = turned[:, j * 128 : (j + 1) * 128]

    def send(src, dst, ssem, rsem, dev):
        return pltpu.make_async_remote_copy(
            src, dst, ssem, rsem, device_id=dev, device_id_type=MESH
        )

    def send_row(k, src, dst, dev):
        return pltpu.make_async_remote_copy(
            src, dst, row_send.at[k], row_recv.at[k], device_id=dev, device_id_type=MESH
        )

    group = 16
    n_group = 128 // group

    def gather(i):
        def fetch(s, k):
            stage[pl.ds((s * group + k) * nlb, nlb), :] = table[bus[i, s * group + k]]

        def pack(s, j):
            g0 = pl.multiple_of(i * 128 + s * group, group)
            got = stage[pl.ds(s * group * nlb + j, group, stride=nlb), :]
            fac[j // (nlb // 2), pl.ds(g0, group), pl.ds((j % (nlb // 2)) * 128, 128)] = got.astype(BF16)

        for k in range(group):
            fetch(0, k)
        for s in range(n_group):
            per = group // nlb
            for j in range(nlb):
                if s + 1 < n_group:
                    for k in range(per):
                        fetch(s + 1, j * per + k)
                pack(s, j)

    steps = gl // 128
    for cp in loads[3:]:
        cp.wait()
    pl.loop(0, steps // 8)(gather)
    yb[0, gen] = yv[...].astype(BF16)
    pl.semaphore_wait(barrier, n_a - 1 + nz - 1 + 4)

    yb_copy = send(yb.at[0, gen], yb.at[0, gen], yb_send, yb_recv, partner)
    yb_copy.start()
    mu_copy = send_row(0, mu_h.at[pl.ds(0, 1)], mu_next, prv)

    @pl.when(tm > 0)
    def _():
        mu_copy.start()

    pl.loop(steps // 8, steps // 2)(gather)
    moves = [
        send(src.at[part], dst.at[part], init_send.at[i], init_recv.at[i], (twin, dev))
        for i, (src, dst, part, dev) in enumerate(
            [(y_h, yt, top, gen), (y_h, yt, low, other), (base_h, bt, top, gen), (base_h, bt, low, other)]
        )
    ]
    moves.append(send(lim_h, lim_x, init_send.at[4], init_recv.at[4], (twin, other)))
    for cp in moves:
        cp.start()

    pl.loop(steps // 2, steps)(gather)
    for cp in loads[:3]:
        cp.wait()

    eye_r = lax.broadcasted_iota(jnp.int32, (rows, rows), 0) == lax.broadcasted_iota(
        jnp.int32, (rows, rows), 1
    )

    def to_column(row):
        return jnp.sum(jnp.where(eye_r, jnp.broadcast_to(row, (rows, rows)), 0.0), axis=1, keepdims=True)

    def to_row(col):
        return jnp.sum(jnp.where(eye_r, jnp.broadcast_to(col, (rows, rows)), 0.0), axis=0, keepdims=True)

    last = tm == ntm - 1
    first = tm == 0
    lam_col = to_column(lam[...])
    dem_col = to_column(dem[...])
    yb_copy.wait()

    @pl.when(tm > 0)
    def _():
        mu_copy.wait_send()

    @pl.when(tm < ntm - 1)
    def _():
        mu_copy.wait_recv()

    muv[pl.ds(rows, 1), :] = jnp.where(last, 0.0, mu_next[...])

    gc = 512
    sums = []
    late = []
    for it in range(ITERS):
        acc_p[...] = jnp.zeros_like(acc_p)
        acc_d[...] = jnp.zeros_like(acc_d)
        acc_t[...] = jnp.zeros_like(acc_t)
        wlam = w * lam_col

        y_t = jnp.concatenate([yb[it, h].astype(F32).T.astype(BF16) for h in range(2)], axis=0)
        for c in range(gl // gc):
            sl = pl.ds(c * gc, gc)
            pulled_t = jnp.dot(fac[0, sl, :], y_t[:half], preferred_element_type=F32) + jnp.dot(
                fac[1, sl, :], y_t[half:], preferred_element_type=F32
            )
            pulled = pulled_t.T
            xc = xv[:, sl]
            grad = cost[:, sl] + wlam + pulled + muv[pl.ds(0, rows), sl] - muv[pl.ds(1, rows), sl]
            xn = jnp.clip(xc - TAU * grad, lo[:, sl], hi[:, sl])
            xb = 2.0 * xn - xc
            d = xn - xc
            d2 = d * d
            xv[:, sl] = xn
            xbv[pl.ds(8, rows), sl] = xb
            edge[it, 0, :, sl] = xb[rows - 1 :]
            if it < ITERS - 1:
                edge[it, 1, :, sl] = xb[:1]
            xbb[:, sl] = xb.astype(BF16)
            acc_p[...] += sum(d2[:, k * 128 : (k + 1) * 128] for k in range(gc // 128))
            acc_t[...] += sum(xb[:, k * 128 : (k + 1) * 128] for k in range(gc // 128))

        rows_out = [send_row(1 + 2 * it, edge.at[it, 0], xb_prev.at[it], nxt)]
        if it < ITERS - 1:
            rows_out.append(send_row(2 + 2 * it, edge.at[it, 1], xb_next, prv))
        has = [tm < ntm - 1, tm > 0]

        @pl.when(has[0])
        def _():
            rows_out[0].start()

        if it < ITERS - 1:

            @pl.when(has[1])
            def _():
                rows_out[1].start()

        tot_col = w * jnp.sum(acc_t[...], axis=1, keepdims=True)
        tot[it, :, pl.ds(0, rows)] = to_row(tot_col)
        t_copy = send(tot.at[it], tot_x.at[it], t_send.at[it], t_recv.at[it], partner)
        t_copy.start()
        f_copies = []
        for p in range(2):
            sums_p = jnp.dot(xbb[...], fac[p], preferred_element_type=F32)
            for r, part in enumerate((top, low)):
                block = sums_p[r * (rows // 2) : (r + 1) * (rows // 2)]
                largest = jnp.maximum(jnp.max(jnp.abs(block), axis=0, keepdims=True), 1e-30)
                flow[it, p, part] = jnp.round(block * (STEPS / largest)).astype(jnp.int32).astype(jnp.int16)
                scale[it, p, r] = largest * (1.0 / STEPS)
                dev = (twin, p if r == 0 else 1 - p)
                for cp in (
                    send(
                        scale.at[it, p, r], scale_x.at[it, gen, r], s_send.at[it, p * 2 + r],
                        s_recv.at[it, gen * 2 + p], dev,
                    ),
                    send(
                        flow.at[it, p, part], frecv.at[it, gen, part], f_send.at[it, p * 2 + r],
                        f_recv.at[it, gen * 2 + p], dev,
                    ),
                ):
                    cp.start()
                    f_copies.append(cp)
        def ramp_pass():
            @pl.when(has[0])
            def _():
                rows_out[0].wait_send()
                if it < ITERS - 1:
                    rows_out[1].wait_recv()

            @pl.when(has[1])
            def _():
                rows_out[0].wait_recv()
                if it < ITERS - 1:
                    rows_out[1].wait_send()

            xbv[pl.ds(7, 1), :] = jnp.where(first, pinit[...], xb_prev[it])
            if it < ITERS - 1:
                m_n = muv[pl.ds(rows, 1), :]
                u_n = m_n + SIGMA * (xb_next[...] - xbv[pl.ds(8 + rows - 1, 1), :])
                mn_n = u_n - jnp.clip(u_n, -SIGMA * ramp[...], SIGMA * ramp[...])
                muv[pl.ds(rows, 1), :] = jnp.where(last, 0.0, mn_n)

            @pl.loop(0, gl // gc)
            def _(c):
                sl = pl.ds(pl.multiple_of(c * gc, gc), gc)
                m = muv[pl.ds(0, rows), sl]
                u = m + SIGMA * (xbv[pl.ds(8, rows), sl] - xbv[pl.ds(7, rows), sl])
                r = SIGMA * ramp[:, sl]
                mn = u - jnp.clip(u, -r, r)
                if it < ITERS - 1:
                    muv[pl.ds(0, rows), sl] = mn
                else:
                    muo[:, sl] = mn
                d = mn - m
                d2 = d * d
                acc_d[...] += sum(d2[:, k * 128 : (k + 1) * 128] for k in range(gc // 128))

        if it == ITERS - 1:
            ramp_pass()
        if it == 0:
            for cp in moves:
                cp.wait()
            lims[other] = lim_x[...]
            lims[gen] = lim[...]
        half_rows = rows // 2
        for p in range(2):
            r = gen if p == 0 else other
            part = pl.ds(pl.multiple_of(r * half_rows, half_rows), half_rows)
            for s in range(2):
                send(
                    scale.at[it, 0, 0], scale_x.at[it, s, r], s_send.at[it, 0], s_recv.at[it, s * 2 + p],
                    (twin, s),
                ).wait_recv()
                send(
                    flow.at[it, 0, top], frecv.at[it, s, part], f_send.at[it, 0], f_recv.at[it, s * 2 + p],
                    (twin, s),
                ).wait_recv()
            old = yt[part, :]
            v = old + SIGMA * sum(
                frecv[it, s, part, :].astype(jnp.int32).astype(F32) * scale_x[it, s, r] for s in range(2)
            )
            bv = bt[part, :]
            lv = lims[p]
            yn = v - jnp.clip(v, SIGMA * (bv - lv), SIGMA * (bv + lv))
            yt[part, :] = yn
            if it < ITERS - 1:
                ybs[part, :] = yn.astype(BF16)
                for dev in range(2):
                    send(
                        ybs.at[part], yb.at[it + 1, p, part], ys_send.at[dev * 2 + p],
                        ys_recv.at[gen * 2 + p], (twin, dev),
                    ).start()
            dy = yn - old
            dy2 = dy * dy
            acc_d[pl.ds(0, half_rows), :] += sum(
                dy2[:, k * 128 : (k + 1) * 128] for k in range(half // 128)
            )
        t_copy.wait()
        totals = tot_col + to_column(tot_x[it, :, pl.ds(0, rows)])
        lam_new = lam_col + SIGMA * (totals - dem_col)
        dl = lam_new - lam_col
        lam_col = lam_new
        late += f_copies
        if it < ITERS - 1:
            ramp_pass()
        primal = jnp.sum(acc_p[...], keepdims=True) / (TAU * cells)
        dual = (
            jnp.sum(acc_d[...], keepdims=True)
            + jnp.where(gen == 0, jnp.sum(dl * dl, keepdims=True), 0.0)
        ) / (SIGMA * cells)
        sums += [primal, dual]
        if it < ITERS - 1:
            for s in range(2):
                for p in range(2):
                    part = top if s == p else low
                    cp = send(
                        ybs.at[part], yb.at[it + 1, p, part], ys_send.at[s * 2 + p],
                        ys_recv.at[s * 2 + p], (twin, s),
                    )
                    cp.wait_recv()
                    late.append(cp)

    lane = lax.broadcasted_iota(jnp.int32, (1, 128), 1)
    packed = jnp.zeros((1, 128), F32)
    for k, s in enumerate(sums):
        packed = jnp.where(lane == k, s, packed)

    def all_sum(value, buf, k, n, mine, peer, between=None):
        msg[k] = value
        buf[mine] = value

        @pl.loop(1, n)
        def _(d):
            pltpu.make_async_remote_copy(
                msg.at[k], buf.at[mine], ar_send.at[k], ar_recv.at[k],
                device_id=peer(d), device_id_type=MESH,
            ).start()

        if between is not None:
            between()
        several = buf.at[pl.ds(0, n - 1)]
        pltpu.make_async_copy(several, several, ar_recv.at[k]).wait()
        return jnp.sum(buf[...], axis=0)

    y_back = [
        send(yt.at[part], yo.at[part], yr_send.at[r], yr_recv.at[r], (twin, dev))
        for r, (part, dev) in enumerate(((top, gen), (low, other)))
    ]

    def return_y():
        for cp in y_back:
            cp.start()

    total = all_sum(packed, ar_a, 0, n_a, mine_a, peer_a, return_y)
    total = all_sum(total, ar_b, 1, nz, zz, peer_b)
    place = 2 * lax.broadcasted_iota(jnp.int32, (ITERS, 2), 0) + lax.broadcasted_iota(
        jnp.int32, (ITERS, 2), 1
    )
    result = jnp.zeros((ITERS, 2), F32)
    for k in range(2 * ITERS):
        one = jnp.sum(jnp.where(lane == k, total, 0.0), axis=1, keepdims=True)
        result = jnp.where(place == k, one, result)
    mov_o[...] = result
    lam_o[...] = to_row(lam_col)
    for cp in y_back:
        cp.wait()
    for cp in late:
        cp.wait_send()
    for k, (buf, n) in enumerate(((ar_a, n_a), (ar_b, nz))):
        several = buf.at[pl.ds(0, n - 1)]
        pltpu.make_async_copy(several, several, ar_send.at[k]).wait()


def write_out(x, y, mu, lam, mov, x_h, y_h, mu_h, lam_h, mov_h, sem):
    copies = [
        pltpu.make_async_copy(s, d, sem.at[i])
        for i, (s, d) in enumerate(((x, x_h), (mu, mu_h), (y, y_h), (lam, lam_h), (mov, mov_h)))
    ]
    for cp in copies:
        cp.start()
    for cp in copies:
        cp.wait()


def on_device(ntm, plane, hours, gl_total,
              dispatch, cost, p_low, p_high, ramp_limit, p_init, demand, bus_of, ptdf, line_base,
              line_limit, line_dual, ramp_dual, balance_dual):
    rows, gl = dispatch.shape
    lines, buses = ptdf.shape
    half = lines // 2
    n_a = 2 * plane
    nz = ntm // plane
    row = lambda a: a.reshape(1, -1)
    hbm = pl.BlockSpec(memory_space=pltpu.HBM)
    vmem = pl.BlockSpec(memory_space=pltpu.VMEM)
    V = pltpu.VMEM
    S = pltpu.SemaphoreType.DMA
    shapes = ((rows, gl), (rows, half), (rows, gl), (1, rows), (ITERS, 2))
    args = (
        bus_of.reshape(-1, 128), dispatch, row(cost), row(p_low), row(p_high), row(ramp_limit), row(p_init),
        row(demand), ptdf, line_base, row(line_limit), line_dual, ramp_dual, row(balance_dual),
    )
    state = pl.pallas_call(
        functools.partial(kernel, (ntm, plane, gl_total, hours)),
        name="dispatch_step",
        out_shape=tuple(V(shape, F32) for shape in shapes),
        in_specs=[hbm] * len(args),
        out_specs=(vmem,) * len(shapes),
        scratch_shapes=[
            V((lines, buses), BF16),
            V((buses, lines // 128, 128), F32),
            V((128 * (lines // 128), 128), F32),
            V((2, gl, half), BF16),
            V((rows + 8, gl), F32),
            V((rows + 8, gl), F32),
            V((rows, gl), BF16),
            V((rows, half), F32),
            V((rows, half), F32),
            V((rows, half), F32),
            V((ITERS, 2, rows, half), jnp.int16),
            V((ITERS, 2, rows, half), BF16),
            V((rows, half), BF16),
            V((ITERS, 2, rows, half), jnp.int16),
            V((ITERS, 2, 2, 1, half), F32), V((ITERS, 2, 2, 1, half), F32),
            pltpu.SMEM((gl // 128, 128), jnp.int32),
            V((1, gl), F32), V((1, gl), F32), V((1, gl), F32), V((1, gl), F32), V((1, gl), F32),
            V((1, half), F32), V((1, half), F32), V((2, 1, half), F32), V((1, rows), F32), V((1, rows), F32),
            V((1, gl), F32), V((ITERS, 2, 1, gl), F32), V((ITERS, 1, gl), F32), V((1, gl), F32), V((ITERS, 1, 128), F32), V((ITERS, 1, 128), F32),
            V((rows, 128), F32), V((rows, 128), F32), V((rows, 128), F32),
            V((2, 1, 128), F32), V((n_a, 1, 128), F32), V((nz, 1, 128), F32),
            S((12,)), S((4,)), S, S, S((5,)), S((5,)), S((ITERS, 4)), S((ITERS, 4)), S((ITERS, 4)), S((ITERS, 4)), S((ITERS,)), S((ITERS,)),
            S((4,)), S((4,)), S((2,)), S((2,)), S((2 * ITERS,)), S((2 * ITERS,)), S((2,)), S((2,)),
        ],
        compiler_params=pltpu.CompilerParams(
            collective_id=0, has_side_effects=True, vmem_limit_bytes=48 * 1024 * 1024
        ),
    )(*(pltpu.with_memory_space_constraint(a, pltpu.HBM) for a in args))
    x, y, mu, lam, mov = pl.pallas_call(
        write_out,
        name="write_out",
        out_shape=tuple(jax.ShapeDtypeStruct(shape, F32) for shape in shapes),
        in_specs=[vmem] * len(shapes),
        out_specs=(hbm,) * len(shapes),
        scratch_shapes=[S((len(shapes),))],
        compiler_params=pltpu.CompilerParams(vmem_limit_bytes=1024 * 1024),
    )(*(pltpu.with_memory_space_constraint(a, pltpu.VMEM) for a in state))
    return x, y, mu, lam.reshape(-1), mov


def solution(mesh):
    ntm = mesh.shape["tm"]
    plane = min(PLANE, ntm)

    def body(*args):
        return on_device(ntm, plane, args[0].shape[0] * ntm, args[0].shape[1] * mesh.shape["gen"], *args)

    in_specs = (
        P("tm", "gen"), P("gen"), P("gen"), P("gen"), P("gen"), P("gen"), P("tm"), P("gen"), P(),
        P("tm", "gen"), P("gen"), P("tm", "gen"), P("tm", "gen"), P("tm"),
    )
    out_specs = (P("tm", "gen"), P("tm", "gen"), P("tm", "gen"), P("tm"), P())
    return jax.shard_map(body, mesh=mesh, in_specs=in_specs, out_specs=out_specs, check_vma=False)
```

```python
import functools
import math

import jax
import jax.numpy as jnp
from jax import lax
from jax.experimental import pallas as pl
from jax.experimental.pallas import tpu as pltpu
from jax.sharding import PartitionSpec as P

TAU = 0.35
SIGMA = 0.35
ITERS = 2
PLANE = 16
MESH = pl.DeviceIdType.MESH
BF16 = jnp.bfloat16
F32 = jnp.float32
STEPS = 32767.0


def kernel(
    cfg,
    bus_h, x_h, cost_h, lo_h, hi_h, ramp_h, pinit_h, dem_h, ptdf_h, base_h, lim_h, y_h, mu_h, lam_h,
    xv, yo, muo, lam_o, mov_o,
    ptdf, table, stage, fac, muv, xbv, xbb, yv, yt, bt, flow, yb, ybs, frecv, scale, scale_x,
    bus, cost, lo, hi, ramp, pinit, lim, lim_x, lims, dem, lam, mu_next, edge, xb_prev, xb_next, tot, tot_x,
    acc_p, acc_d, acc_t, msg, ar_a, ar_b,
    load_sem, ptdf_sem, yb_send, yb_recv, init_send, init_recv, f_send, f_recv, s_send, s_recv, t_send, t_recv,
    ys_send, ys_recv, yr_send, yr_recv, row_send, row_recv, ar_send, ar_recv,
):
    ntm, plane, gl_total, hours = cfg
    rows, gl = x_h.shape
    lines, buses = ptdf_h.shape
    half = lines // 2
    nz = ntm // plane
    w = 1.0 / math.sqrt(gl_total)
    cells = float(hours) * float(gl_total)
    tm = lax.axis_index("tm")
    gen = lax.axis_index("gen")
    other = 1 - gen
    partner = (tm, other)
    nxt = (lax.rem(tm + 1, ntm), gen)
    prv = (lax.rem(tm + ntm - 1, ntm), gen)
    twin = tm + 2 - 4 * lax.rem(tm // 2, 2)
    top = pl.ds(0, rows // 2)
    low = pl.ds(rows // 2, rows // 2)
    zz = tm // plane
    in_plane = lax.rem(tm, plane)
    n_a = 2 * plane
    mine_a = in_plane * 2 + gen

    def peer_a(d):
        q = lax.rem(mine_a + d, n_a)
        return (zz * plane + q // 2, lax.rem(q, 2))

    def peer_b(d):
        return (lax.rem(zz + d, nz) * plane + in_plane, gen)

    nblk = buses // 256
    n_load = min(4, nblk)
    per_load = nblk // n_load
    ptdf_copies = []
    for c in range(n_load):
        part = pl.ds(c * per_load * 256, per_load * 256)
        cp = pltpu.make_async_copy(ptdf_h.at[:, part], ptdf.at[:, part], ptdf_sem.at[c])
        cp.start()
        ptdf_copies.append(cp)
    loads = [
        pltpu.make_async_copy(s, d, load_sem.at[i])
        for i, (s, d) in enumerate(
            [
                (mu_h, muv.at[pl.ds(0, rows)]), (x_h, xv), (cost_h, cost), (y_h, yv),
                (lo_h, lo), (hi_h, hi), (ramp_h, ramp), (pinit_h, pinit), (lim_h, lim), (dem_h, dem),
                (lam_h, lam), (bus_h, bus),
            ]
        )
    ]
    for cp in loads[3:]:
        cp.start()

    barrier = pltpu.get_barrier_semaphore()

    def greet(dev):
        pl.semaphore_signal(barrier, inc=1, device_id=dev, device_id_type=MESH)

    greet(nxt)
    greet(prv)
    greet((twin, 0))
    greet((twin, 1))

    @pl.loop(1, n_a)
    def _(d):
        greet(peer_a(d))

    @pl.loop(1, nz)
    def _(d):
        greet(peer_b(d))

    nlb = lines // 128
    flat = table.reshape(buses * nlb, 128)
    for c in range(nblk):
        if c % per_load == 0:
            ptdf_copies[c // per_load].wait()
            if c // per_load == n_load - 1:
                for cp in loads[:3]:
                    cp.start()
        turned = ptdf[:, c * 256 : (c + 1) * 256].T.astype(F32)
        for j in range(nlb):
            flat[pl.ds(c * 256 * nlb + j, 256, stride=nlb), :] = turned[:, j * 128 : (j + 1) * 128]

    def send(src, dst, ssem, rsem, dev):
        return pltpu.make_async_remote_copy(
            src, dst, ssem, rsem, device_id=dev, device_id_type=MESH
        )

    def send_row(k, src, dst, dev):
        return pltpu.make_async_remote_copy(
            src, dst, row_send.at[k], row_recv.at[k], device_id=dev, device_id_type=MESH
        )

    group = 16
    n_group = 128 // group

    def gather(i):
        def fetch(s, k):
            stage[pl.ds((s * group + k) * nlb, nlb), :] = table[bus[i, s * group + k]]

        def pack(s, j):
            g0 = pl.multiple_of(i * 128 + s * group, group)
            got = stage[pl.ds(s * group * nlb + j, group, stride=nlb), :]
            fac[j // (nlb // 2), pl.ds(g0, group), pl.ds((j % (nlb // 2)) * 128, 128)] = got.astype(BF16)

        for k in range(group):
            fetch(0, k)
        for s in range(n_group):
            per = group // nlb
            for j in range(nlb):
                if s + 1 < n_group:
                    for k in range(per):
                        fetch(s + 1, j * per + k)
                pack(s, j)

    steps = gl // 128
    for cp in loads[3:]:
        cp.wait()
    pl.loop(0, steps // 8)(gather)
    yb[0, gen] = yv[...].astype(BF16)
    pl.semaphore_wait(barrier, n_a - 1 + nz - 1 + 4)

    yb_copy = send(yb.at[0, gen], yb.at[0, gen], yb_send, yb_recv, partner)
    yb_copy.start()
    mu_copy = send_row(0, mu_h.at[pl.ds(0, 1)], mu_next, prv)

    @pl.when(tm > 0)
    def _():
        mu_copy.start()

    pl.loop(steps // 8, steps // 2)(gather)
    moves = [
        send(src.at[part], dst.at[part], init_send.at[i], init_recv.at[i], (twin, dev))
        for i, (src, dst, part, dev) in enumerate(
            [(y_h, yt, top, gen), (y_h, yt, low, other), (base_h, bt, top, gen), (base_h, bt, low, other)]
        )
    ]
    moves.append(send(lim_h, lim_x, init_send.at[4], init_recv.at[4], (twin, other)))
    for cp in moves:
        cp.start()

    pl.loop(steps // 2, steps)(gather)
    for cp in loads[:3]:
        cp.wait()

    eye_r = lax.broadcasted_iota(jnp.int32, (rows, rows), 0) == lax.broadcasted_iota(
        jnp.int32, (rows, rows), 1
    )

    def to_column(row):
        return jnp.sum(jnp.where(eye_r, jnp.broadcast_to(row, (rows, rows)), 0.0), axis=1, keepdims=True)

    def to_row(col):
        return jnp.sum(jnp.where(eye_r, jnp.broadcast_to(col, (rows, rows)), 0.0), axis=0, keepdims=True)

    last = tm == ntm - 1
    first = tm == 0
    lam_col = to_column(lam[...])
    dem_col = to_column(dem[...])
    yb_copy.wait()

    @pl.when(tm > 0)
    def _():
        mu_copy.wait_send()

    @pl.when(tm < ntm - 1)
    def _():
        mu_copy.wait_recv()

    muv[pl.ds(rows, 1), :] = jnp.where(last, 0.0, mu_next[...])

    gc = 1024
    sums = []
    late = []
    for it in range(ITERS):
        acc_p[...] = jnp.zeros_like(acc_p)
        acc_d[...] = jnp.zeros_like(acc_d)
        acc_t[...] = jnp.zeros_like(acc_t)
        wlam = w * lam_col

        y_t = jnp.concatenate([yb[it, h].astype(F32).T.astype(BF16) for h in range(2)], axis=0)
        for c in range(gl // gc):
            sl = pl.ds(c * gc, gc)
            pulled_t = jnp.dot(fac[0, sl, :], y_t[:half], preferred_element_type=F32) + jnp.dot(
                fac[1, sl, :], y_t[half:], preferred_element_type=F32
            )
            pulled = pulled_t.T
            xc = xv[:, sl]
            grad = cost[:, sl] + wlam + pulled + muv[pl.ds(0, rows), sl] - muv[pl.ds(1, rows), sl]
            xn = jnp.clip(xc - TAU * grad, lo[:, sl], hi[:, sl])
            xb = 2.0 * xn - xc
            d = xn - xc
            d2 = d * d
            xv[:, sl] = xn
            xbv[pl.ds(8, rows), sl] = xb
            edge[it, 0, :, sl] = xb[rows - 1 :]
            if it < ITERS - 1:
                edge[it, 1, :, sl] = xb[:1]
            xbb[:, sl] = xb.astype(BF16)
            acc_p[...] += sum(d2[:, k * 128 : (k + 1) * 128] for k in range(gc // 128))
            acc_t[...] += sum(xb[:, k * 128 : (k + 1) * 128] for k in range(gc // 128))

        rows_out = [send_row(1 + 2 * it, edge.at[it, 0], xb_prev.at[it], nxt)]
        if it < ITERS - 1:
            rows_out.append(send_row(2 + 2 * it, edge.at[it, 1], xb_next, prv))
        has = [tm < ntm - 1, tm > 0]

        @pl.when(has[0])
        def _():
            rows_out[0].start()

        if it < ITERS - 1:

            @pl.when(has[1])
            def _():
                rows_out[1].start()

        tot_col = w * jnp.sum(acc_t[...], axis=1, keepdims=True)
        tot[it, :, pl.ds(0, rows)] = to_row(tot_col)
        t_copy = send(tot.at[it], tot_x.at[it], t_send.at[it], t_recv.at[it], partner)
        t_copy.start()
        f_copies = []
        for p in range(2):
            sums_p = jnp.dot(xbb[...], fac[p], preferred_element_type=F32)
            for r, part in enumerate((top, low)):
                block = sums_p[r * (rows // 2) : (r + 1) * (rows // 2)]
                largest = jnp.maximum(jnp.max(jnp.abs(block), axis=0, keepdims=True), 1e-30)
                flow[it, p, part] = jnp.round(block * (STEPS / largest)).astype(jnp.int32).astype(jnp.int16)
                scale[it, p, r] = largest * (1.0 / STEPS)
                dev = (twin, p if r == 0 else 1 - p)
                for cp in (
                    send(
                        scale.at[it, p, r], scale_x.at[it, gen, r], s_send.at[it, p * 2 + r],
                        s_recv.at[it, gen * 2 + p], dev,
                    ),
                    send(
                        flow.at[it, p, part], frecv.at[it, gen, part], f_send.at[it, p * 2 + r],
                        f_recv.at[it, gen * 2 + p], dev,
                    ),
                ):
                    cp.start()
                    f_copies.append(cp)
        def ramp_pass():
            @pl.when(has[0])
            def _():
                rows_out[0].wait_send()
                if it < ITERS - 1:
                    rows_out[1].wait_recv()

            @pl.when(has[1])
            def _():
                rows_out[0].wait_recv()
                if it < ITERS - 1:
                    rows_out[1].wait_send()

            xbv[pl.ds(7, 1), :] = jnp.where(first, pinit[...], xb_prev[it])
            if it < ITERS - 1:
                m_n = muv[pl.ds(rows, 1), :]
                u_n = m_n + SIGMA * (xb_next[...] - xbv[pl.ds(8 + rows - 1, 1), :])
                mn_n = u_n - jnp.clip(u_n, -SIGMA * ramp[...], SIGMA * ramp[...])
                muv[pl.ds(rows, 1), :] = jnp.where(last, 0.0, mn_n)

            @pl.loop(0, gl // gc)
            def _(c):
                sl = pl.ds(pl.multiple_of(c * gc, gc), gc)
                m = muv[pl.ds(0, rows), sl]
                u = m + SIGMA * (xbv[pl.ds(8, rows), sl] - xbv[pl.ds(7, rows), sl])
                r = SIGMA * ramp[:, sl]
                mn = u - jnp.clip(u, -r, r)
                if it < ITERS - 1:
                    muv[pl.ds(0, rows), sl] = mn
                else:
                    muo[:, sl] = mn
                d = mn - m
                d2 = d * d
                acc_d[...] += sum(d2[:, k * 128 : (k + 1) * 128] for k in range(gc // 128))

        if it == ITERS - 1:
            ramp_pass()
        if it == 0:
            for cp in moves:
                cp.wait()
            lims[other] = lim_x[...]
            lims[gen] = lim[...]
        half_rows = rows // 2
        for p in range(2):
            r = gen if p == 0 else other
            part = pl.ds(pl.multiple_of(r * half_rows, half_rows), half_rows)
            for s in range(2):
                send(
                    scale.at[it, 0, 0], scale_x.at[it, s, r], s_send.at[it, 0], s_recv.at[it, s * 2 + p],
                    (twin, s),
                ).wait_recv()
                send(
                    flow.at[it, 0, top], frecv.at[it, s, part], f_send.at[it, 0], f_recv.at[it, s * 2 + p],
                    (twin, s),
                ).wait_recv()
            old = yt[part, :]
            v = old + SIGMA * sum(
                frecv[it, s, part, :].astype(jnp.int32).astype(F32) * scale_x[it, s, r] for s in range(2)
            )
            bv = bt[part, :]
            lv = lims[p]
            yn = v - jnp.clip(v, SIGMA * (bv - lv), SIGMA * (bv + lv))
            yt[part, :] = yn
            if it < ITERS - 1:
                ybs[part, :] = yn.astype(BF16)
                for dev in range(2):
                    send(
                        ybs.at[part], yb.at[it + 1, p, part], ys_send.at[dev * 2 + p],
                        ys_recv.at[gen * 2 + p], (twin, dev),
                    ).start()
            dy = yn - old
            dy2 = dy * dy
            acc_d[pl.ds(0, half_rows), :] += sum(
                dy2[:, k * 128 : (k + 1) * 128] for k in range(half // 128)
            )
        t_copy.wait()
        totals = tot_col + to_column(tot_x[it, :, pl.ds(0, rows)])
        lam_new = lam_col + SIGMA * (totals - dem_col)
        dl = lam_new - lam_col
        lam_col = lam_new
        late += f_copies
        if it < ITERS - 1:
            ramp_pass()
        primal = jnp.sum(acc_p[...], keepdims=True) / (TAU * cells)
        dual = (
            jnp.sum(acc_d[...], keepdims=True)
            + jnp.where(gen == 0, jnp.sum(dl * dl, keepdims=True), 0.0)
        ) / (SIGMA * cells)
        sums += [primal, dual]
        if it < ITERS - 1:
            for s in range(2):
                for p in range(2):
                    part = top if s == p else low
                    cp = send(
                        ybs.at[part], yb.at[it + 1, p, part], ys_send.at[s * 2 + p],
                        ys_recv.at[s * 2 + p], (twin, s),
                    )
                    cp.wait_recv()
                    late.append(cp)

    lane = lax.broadcasted_iota(jnp.int32, (1, 128), 1)
    packed = jnp.zeros((1, 128), F32)
    for k, s in enumerate(sums):
        packed = jnp.where(lane == k, s, packed)

    def all_sum(value, buf, k, n, mine, peer, between=None):
        msg[k] = value
        buf[mine] = value

        @pl.loop(1, n)
        def _(d):
            pltpu.make_async_remote_copy(
                msg.at[k], buf.at[mine], ar_send.at[k], ar_recv.at[k],
                device_id=peer(d), device_id_type=MESH,
            ).start()

        if between is not None:
            between()
        several = buf.at[pl.ds(0, n - 1)]
        pltpu.make_async_copy(several, several, ar_recv.at[k]).wait()
        return jnp.sum(buf[...], axis=0)

    y_back = [
        send(yt.at[part], yo.at[part], yr_send.at[r], yr_recv.at[r], (twin, dev))
        for r, (part, dev) in enumerate(((top, gen), (low, other)))
    ]

    def return_y():
        for cp in y_back:
            cp.start()

    total = all_sum(packed, ar_a, 0, n_a, mine_a, peer_a, return_y)
    total = all_sum(total, ar_b, 1, nz, zz, peer_b)
    place = 2 * lax.broadcasted_iota(jnp.int32, (ITERS, 2), 0) + lax.broadcasted_iota(
        jnp.int32, (ITERS, 2), 1
    )
    result = jnp.zeros((ITERS, 2), F32)
    for k in range(2 * ITERS):
        one = jnp.sum(jnp.where(lane == k, total, 0.0), axis=1, keepdims=True)
        result = jnp.where(place == k, one, result)
    mov_o[...] = result
    lam_o[...] = to_row(lam_col)
    for cp in y_back:
        cp.wait()
    for cp in late:
        cp.wait_send()
    for k, (buf, n) in enumerate(((ar_a, n_a), (ar_b, nz))):
        several = buf.at[pl.ds(0, n - 1)]
        pltpu.make_async_copy(several, several, ar_send.at[k]).wait()


def write_out(x, y, mu, lam, mov, x_h, y_h, mu_h, lam_h, mov_h, sem):
    copies = [
        pltpu.make_async_copy(s, d, sem.at[i])
        for i, (s, d) in enumerate(((x, x_h), (mu, mu_h), (y, y_h), (lam, lam_h), (mov, mov_h)))
    ]
    for cp in copies:
        cp.start()
    for cp in copies:
        cp.wait()


def on_device(ntm, plane, hours, gl_total,
              dispatch, cost, p_low, p_high, ramp_limit, p_init, demand, bus_of, ptdf, line_base,
              line_limit, line_dual, ramp_dual, balance_dual):
    rows, gl = dispatch.shape
    lines, buses = ptdf.shape
    half = lines // 2
    n_a = 2 * plane
    nz = ntm // plane
    row = lambda a: a.reshape(1, -1)
    hbm = pl.BlockSpec(memory_space=pltpu.HBM)
    vmem = pl.BlockSpec(memory_space=pltpu.VMEM)
    V = pltpu.VMEM
    S = pltpu.SemaphoreType.DMA
    shapes = ((rows, gl), (rows, half), (rows, gl), (1, rows), (ITERS, 2))
    args = (
        bus_of.reshape(-1, 128), dispatch, row(cost), row(p_low), row(p_high), row(ramp_limit), row(p_init),
        row(demand), ptdf, line_base, row(line_limit), line_dual, ramp_dual, row(balance_dual),
    )
    state = pl.pallas_call(
        functools.partial(kernel, (ntm, plane, gl_total, hours)),
        name="dispatch_step",
        out_shape=tuple(V(shape, F32) for shape in shapes),
        in_specs=[hbm] * len(args),
        out_specs=(vmem,) * len(shapes),
        scratch_shapes=[
            V((lines, buses), BF16),
            V((buses, lines // 128, 128), F32),
            V((128 * (lines // 128), 128), F32),
            V((2, gl, half), BF16),
            V((rows + 8, gl), F32),
            V((rows + 8, gl), F32),
            V((rows, gl), BF16),
            V((rows, half), F32),
            V((rows, half), F32),
            V((rows, half), F32),
            V((ITERS, 2, rows, half), jnp.int16),
            V((ITERS, 2, rows, half), BF16),
            V((rows, half), BF16),
            V((ITERS, 2, rows, half), jnp.int16),
            V((ITERS, 2, 2, 1, half), F32), V((ITERS, 2, 2, 1, half), F32),
            pltpu.SMEM((gl // 128, 128), jnp.int32),
            V((1, gl), F32), V((1, gl), F32), V((1, gl), F32), V((1, gl), F32), V((1, gl), F32),
            V((1, half), F32), V((1, half), F32), V((2, 1, half), F32), V((1, rows), F32), V((1, rows), F32),
            V((1, gl), F32), V((ITERS, 2, 1, gl), F32), V((ITERS, 1, gl), F32), V((1, gl), F32), V((ITERS, 1, 128), F32), V((ITERS, 1, 128), F32),
            V((rows, 128), F32), V((rows, 128), F32), V((rows, 128), F32),
            V((2, 1, 128), F32), V((n_a, 1, 128), F32), V((nz, 1, 128), F32),
            S((12,)), S((4,)), S, S, S((5,)), S((5,)), S((ITERS, 4)), S((ITERS, 4)), S((ITERS, 4)), S((ITERS, 4)), S((ITERS,)), S((ITERS,)),
            S((4,)), S((4,)), S((2,)), S((2,)), S((2 * ITERS,)), S((2 * ITERS,)), S((2,)), S((2,)),
        ],
        compiler_params=pltpu.CompilerParams(
            collective_id=0, has_side_effects=True, vmem_limit_bytes=48 * 1024 * 1024
        ),
    )(*(pltpu.with_memory_space_constraint(a, pltpu.HBM) for a in args))
    x, y, mu, lam, mov = pl.pallas_call(
        write_out,
        name="write_out",
        out_shape=tuple(jax.ShapeDtypeStruct(shape, F32) for shape in shapes),
        in_specs=[vmem] * len(shapes),
        out_specs=(hbm,) * len(shapes),
        scratch_shapes=[S((len(shapes),))],
        compiler_params=pltpu.CompilerParams(vmem_limit_bytes=1024 * 1024),
    )(*(pltpu.with_memory_space_constraint(a, pltpu.VMEM) for a in state))
    return x, y, mu, lam.reshape(-1), mov


def solution(mesh):
    ntm = mesh.shape["tm"]
    plane = min(PLANE, ntm)

    def body(*args):
        return on_device(ntm, plane, args[0].shape[0] * ntm, args[0].shape[1] * mesh.shape["gen"], *args)

    in_specs = (
        P("tm", "gen"), P("gen"), P("gen"), P("gen"), P("gen"), P("gen"), P("tm"), P("gen"), P(),
        P("tm", "gen"), P("gen"), P("tm", "gen"), P("tm", "gen"), P("tm"),
    )
    out_specs = (P("tm", "gen"), P("tm", "gen"), P("tm", "gen"), P("tm"), P())
    return jax.shard_map(body, mesh=mesh, in_specs=in_specs, out_specs=out_specs, check_vma=False)
```
